64 devices in a mesh: dp: 4 (over x, y), tp: 16 (over z, core).
Axes of the slice: x: 2, y: 2, z: 8, core: 2. Of those that a mesh axis runs over, the one named last changes fastest.
The devices are a block of a 4x4x8 slice.
Arguments:
- token_ids: int32 [4096], P('dp'), parts along dimension 0
- embed_table: bfloat16 [32000, 4096], P('tp')
- norm_gain: bfloat16 [4096], replicated
- w_in: bfloat16 [4096, 11008], P(None, 'tp')
- w_out: bfloat16 [11008, 4096], P('tp')
Outputs:
- output: bfloat16 [4096, 4096], P(('dp', 'tp')), parts along dimension 0
There are 4 independent parts. The reference program is written for one: setup_inputs(seed, part) draws one part's arguments, and reference() takes and returns one part's arrays. A program takes and returns all parts, laid end to end along the dimension named above; an argument that names none is the same for every part.
All inputs are finite; a program needn't handle non-finite values.
Results may differ from the reference program's by a relative error of at most 0.00792369.
Values are sent between devices in bfloat16 or wider.
A program may use at most 768 MiB of HBM per device.

```python
import math
import jax
import jax.numpy as jnp
from jax import lax

TOKENS = 1024
VOCAB_SIZE = 32000
MODEL_DIM = 4096
MLP_WIDTH = 11008
RMS_EPS = 1e-6
ROW_BLOCK = math.gcd(TOKENS, 256)


def draw_token_ids(key):
    key_mix, key_low, key_all, key_first, key_last = jax.random.split(key, 5)
    choose_low = jax.random.randint(key_mix, (TOKENS,), 0, 4) == 0
    low_ids = jax.random.randint(key_low, (TOKENS,), 0, VOCAB_SIZE // 8)
    any_ids = jax.random.randint(key_all, (TOKENS,), 0, VOCAB_SIZE)
    token_ids = jnp.where(choose_low, low_ids, any_ids)
    first_pos = jax.random.randint(key_first, (), 0, TOKENS // 2)
    last_pos = jax.random.randint(key_last, (), TOKENS // 2, TOKENS)
    token_ids = token_ids.at[first_pos].set(0).at[last_pos].set(VOCAB_SIZE - 1)
    return token_ids.astype(jnp.int32)


def setup_inputs(seed: int = 0, part: int = 0) -> dict:
    base_key = jax.random.key(seed)
    key_ids = jax.random.fold_in(jax.random.fold_in(base_key, 1), part)
    key_table, key_gain, key_in, key_out = jax.random.split(jax.random.fold_in(base_key, 2), 4)
    embed_table = jax.random.normal(key_table, (VOCAB_SIZE, MODEL_DIM), jnp.float32)
    norm_gain = jax.random.uniform(key_gain, (MODEL_DIM,), jnp.float32, 0.5, 1.5)
    w_in = jax.random.normal(key_in, (MODEL_DIM, MLP_WIDTH), jnp.float32) * MODEL_DIM ** -0.5
    w_out = jax.random.normal(key_out, (MLP_WIDTH, MODEL_DIM), jnp.float32) * MLP_WIDTH ** -0.5
    return {
        "token_ids": draw_token_ids(key_ids),
        "embed_table": embed_table.astype(jnp.bfloat16),
        "norm_gain": norm_gain.astype(jnp.bfloat16),
        "w_in": w_in.astype(jnp.bfloat16),
        "w_out": w_out.astype(jnp.bfloat16),
    }


def block_forward(embed_rows, norm_gain, w_in, w_out):
    rows_f32 = embed_rows.astype(jnp.float32)
    inv_rms = lax.rsqrt(jnp.mean(rows_f32 * rows_f32, axis=-1, keepdims=True) + RMS_EPS)
    normed = (rows_f32 * inv_rms * norm_gain.astype(jnp.float32)).astype(jnp.bfloat16)
    pre_act = jnp.dot(normed, w_in, preferred_element_type=jnp.float32).astype(jnp.bfloat16)
    activated = jax.nn.gelu(pre_act.astype(jnp.float32), approximate=True).astype(jnp.bfloat16)
    mlp_sum = jnp.dot(activated, w_out, preferred_element_type=jnp.float32)
    return (rows_f32 + mlp_sum).astype(jnp.bfloat16)


def reference(token_ids, embed_table, norm_gain, w_in, w_out):
    embedded = jnp.take(embed_table, token_ids, axis=0)
    row_blocks = embedded.reshape(TOKENS // ROW_BLOCK, ROW_BLOCK, MODEL_DIM)
    outputs = lax.map(lambda row_blk: block_forward(row_blk, norm_gain, w_in, w_out), row_blocks)
    return outputs.reshape(TOKENS, MODEL_DIM)
```

```python
import functools

import jax
import jax.numpy as jnp
from jax import lax
from jax.experimental import pallas as pl
from jax.experimental.pallas import tpu as pltpu
from jax.sharding import PartitionSpec as P

MESH = pl.DeviceIdType.MESH
RMS_EPS = 1e-6
CORES = 2
HALVES = 2
VMEM_BYTES = 67043328


def block_kernel(
    group, ids_ref, table_hbm, gain_ref, w1_hbm, w2_hbm, out_ref,
    table, w1, w2, onehot, xa, x_own, p1send, r1send,
    ymine, ysend, ypart, r2recv, r2send,
    load_sem, w_sem, p1_ssem, p1_rsem, r1_ssem, r1_rsem,
    ag_ssem, ag_rsem, agp_ssem, agp_rsem, yp_ssem, yp_rsem, r2_ssem, r2_rsem,
    credit_ring, credit_core,
):
    ring = group // CORES
    me = lax.axis_index("tp")
    z, core = me // CORES, me % CORES
    step_dir = 1 - 2 * core
    nxt = lax.rem(z + step_dir + ring, ring) * CORES + core
    prv = lax.rem(z - step_dir + ring, ring) * CORES + core
    mate = z * CORES + (1 - core)

    block = out_ref.shape[0]
    half_w = xa.shape[3]
    vocab = table_hbm.shape[0]
    vocab_pad = table.shape[0]
    tile_g = min(512, half_w)
    tile_y = min(512, half_w)
    tiles = half_w * HALVES // tile_g

    def remote(src, dst, ssem, rsem, dev):
        return pltpu.make_async_remote_copy(
            src_ref=src, dst_ref=dst, send_sem=ssem, recv_sem=rsem,
            device_id={"tp": dev}, device_id_type=MESH,
        )

    def table_load(j):
        cols = pl.ds(j * tile_g, tile_g)
        return pltpu.make_async_copy(
            table_hbm.at[:, cols], table.at[pl.ds(0, vocab), cols], load_sem.at[j]
        )

    for j in range(tiles):
        table_load(j).start()

    barrier = pltpu.get_barrier_semaphore()
    for dev in (nxt, prv, mate):
        pl.semaphore_signal(barrier, inc=1, device_id={"tp": dev}, device_id_type=MESH)

    if vocab_pad > vocab:
        table[vocab:, :] = jnp.zeros((vocab_pad - vocab, table.shape[1]), table.dtype)
    pl.semaphore_wait(barrier, 3)

    def w1_load():
        return pltpu.make_async_copy(w1_hbm, w1, w_sem.at[0])

    def w2_load():
        return pltpu.make_async_copy(w2_hbm, w2, w_sem.at[1])

    def p1_copy(t, h):
        return remote(
            p1send.at[h], xa.at[t, h, pl.ds(block, block)],
            p1_ssem.at[h], p1_rsem.at[t, h], mate,
        )

    def r1_copy(t, h):
        return remote(
            r1send.at[t % 2, h], xa.at[t, h, pl.ds(0, block)],
            r1_ssem.at[t % 2, h], r1_rsem.at[t, h], nxt,
        )

    def chip_back(s):
        return lax.rem(z - step_dir * s + 2 * ring, ring)

    def chip_ahead(s):
        return lax.rem(z + step_dir * s + 2 * ring, ring)

    def fill_onehot(t):
        for row, chip, c in ((0, chip_back(1 + t), core), (block, chip_ahead(1 + t), 1 - core)):
            first = pl.multiple_of((chip * CORES + c) * block, block)
            local = ids_ref[pl.ds(first, block), :] - me * vocab
            slots = lax.broadcasted_iota(jnp.int32, (block, vocab_pad), 1)
            hit = jnp.where((slots == local) & (slots < vocab), 1.0, 0.0)
            onehot[pl.ds(row, block), :] = hit.astype(jnp.bfloat16)

    def gather_half(t, h):
        for j in range(half_w // tile_g):
            g = h * (half_w // tile_g) + j

            @pl.when(t == 0)
            def _():
                table_load(g).wait()

            rows = jnp.dot(
                onehot[...], table[:, g * tile_g:(g + 1) * tile_g],
                preferred_element_type=jnp.float32,
            ).astype(jnp.bfloat16)
            cols = slice(j * tile_g, (j + 1) * tile_g)
            x_own[h, :, cols] = rows[:block]
            p1send[h, :, cols] = rows[block:]

    def ring1_half(t, h):
        p1_copy(t, h).wait_recv()

        @pl.when(t >= 2)
        def _():
            r1_copy(t - 2, h).wait_send()

        r1send[t % 2, h] = x_own[h] + xa[t, h, block:]

        @pl.when(t >= 1)
        def _():
            r1_copy(t - 1, h).wait_recv()
            r1send[t % 2, h] = r1send[t % 2, h] + xa[t - 1, h, :block]

        r1_copy(t, h).start()

    def rows_step(t, carry):
        fill_onehot(t)

        @pl.when(t == 1)
        def _():
            w1_load().start()
            w2_load().start()

        for h in range(HALVES):
            @pl.when(t >= 1)
            def _():
                ring1_half(t - 1, h)

            @pl.when(t >= 1)
            def _():
                p1_copy(t - 1, h).wait_send()

            gather_half(t, h)
            p1_copy(t, h).start()
        return carry

    lax.fori_loop(0, ring, rows_step, 0)

    last = ring - 1
    for h in range(HALVES):
        p1_copy(last, h).wait_recv()
        r1_copy(last - 1, h).wait_recv()
        x_own[h] = x_own[h] + xa[last, h, block:] + xa[last - 1, h, :block]
    pl.semaphore_signal(credit_ring, inc=1, device_id={"tp": prv}, device_id_type=MESH)
    pl.semaphore_signal(credit_core, inc=1, device_id={"tp": mate}, device_id_type=MESH)

    total = jnp.zeros((block, 1), jnp.float32)
    for h in range(HALVES):
        xf = x_own[h].astype(jnp.float32)
        total = total + jnp.sum(xf * xf, axis=-1, keepdims=True)
    inv_rms = lax.rsqrt(total / (half_w * HALVES) + RMS_EPS)
    for h in range(HALVES):
        gain = gain_ref[:, h * half_w:(h + 1) * half_w].astype(jnp.float32)
        xa[0, h, :block] = (x_own[h].astype(jnp.float32) * inv_rms * gain).astype(jnp.bfloat16)

    def ag_copy(s, h):
        return remote(
            xa.at[s, h, pl.ds(0, block)], xa.at[s + 1, h, pl.ds(0, block)],
            ag_ssem.at[s, h], ag_rsem.at[s, h], nxt,
        )

    def agp_copy(s, h):
        return remote(
            xa.at[s, h, pl.ds(0, block)], xa.at[s, h, pl.ds(block, block)],
            agp_ssem.at[s, h], agp_rsem.at[s, h], mate,
        )

    def yp_copy(s, h):
        return remote(
            ysend.at[h], ypart.at[s, h],
            yp_ssem.at[h], yp_rsem.at[s, h], mate,
        )

    def r2_copy(s, h):
        return remote(
            r2send.at[s % 2, h], r2recv.at[s - 1, h],
            r2_ssem.at[s % 2, h], r2_rsem.at[s - 1, h], nxt,
        )

    pl.semaphore_wait(credit_ring, 1)
    pl.semaphore_wait(credit_core, 1)
    w1_load().wait()
    w2_load().wait()

    def mlp_step(s, carry):
        for h in range(HALVES):
            @pl.when(s >= 1)
            def _():
                ag_copy(s - 1, h).wait_recv()

            @pl.when(s < ring - 1)
            def _():
                ag_copy(s, h).start()

            agp_copy(s, h).start()

        acc = None
        for h in range(HALVES):
            agp_copy(s, h).wait_recv()
            part = lax.dot_general(
                xa[s, h], w1[:, h * half_w:(h + 1) * half_w], (((1,), (1,)), ((), ())),
                preferred_element_type=jnp.float32,
            )
            acc = part if acc is None else acc + part
        u = acc.astype(jnp.bfloat16).astype(jnp.float32)
        act = jax.nn.gelu(u, approximate=True).astype(jnp.bfloat16)

        kept = jnp.minimum(s, 1)
        for h in range(HALVES):
            @pl.when(s >= 1)
            def _():
                yp_copy(s - 1, h).wait_send()

            for j in range(half_w // tile_y):
                c0 = h * half_w + j * tile_y
                y = jnp.dot(act, w2[:, c0:c0 + tile_y], preferred_element_type=jnp.float32)
                cols = slice(j * tile_y, (j + 1) * tile_y)
                ymine[kept, h, :, cols] = y[:block]
                ysend[h, :, cols] = y[block:]
            yp_copy(s, h).start()

        @pl.when(s >= 1)
        def _():
            for h in range(HALVES):
                yp_copy(s, h).wait_recv()

                @pl.when(s >= 3)
                def _():
                    r2_copy(s - 2, h).wait_send()

                r2send[s % 2, h] = ymine[1, h] + ypart[s, h]

                @pl.when(s >= 2)
                def _():
                    r2_copy(s - 1, h).wait_recv()
                    r2send[s % 2, h] = r2send[s % 2, h] + r2recv[s - 2, h]

                r2_copy(s, h).start()
        return carry

    lax.fori_loop(0, ring, mlp_step, 0)

    for h in range(HALVES):
        yp_copy(0, h).wait_recv()
        r2_copy(ring - 1, h).wait_recv()
        own = ymine[0, h] + ypart[0, h] + r2recv[ring - 2, h]
        out_ref[:, h * half_w:(h + 1) * half_w] = (
            x_own[h].astype(jnp.float32) + own
        ).astype(jnp.bfloat16)

    for h in range(HALVES):
        p1_copy(last, h).wait_send()
        yp_copy(last, h).wait_send()
        for t in (ring - 2, ring - 1):
            r1_copy(t - 1, h).wait_send()
            r2_copy(t, h).wait_send()
        for s in range(ring):
            agp_copy(s, h).wait_send()
            if s < ring - 1:
                ag_copy(s, h).wait_send()


def solution(mesh):
    group = mesh.shape["tp"]
    ring = group // CORES

    def device_step(token_ids, table_shard, norm_gain, w_in_shard, w_out_shard):
        tokens = token_ids.shape[0]
        vocab, dim = table_shard.shape
        width = w_in_shard.shape[1]
        block, half_w = tokens // group, dim // HALVES
        vocab_pad = -(-vocab // 256) * 256
        bf16, f32 = jnp.bfloat16, jnp.float32
        dma = pltpu.SemaphoreType.DMA
        vmem = pl.BlockSpec(memory_space=pltpu.VMEM)
        hbm = pl.BlockSpec(memory_space=pl.ANY)
        return pl.pallas_call(
            functools.partial(block_kernel, group),
            name="lookup_mlp",
            out_shape=jax.ShapeDtypeStruct((block, dim), bf16),
            in_specs=[vmem, hbm, vmem, hbm, hbm],
            out_specs=vmem,
            scratch_shapes=[
                pltpu.VMEM((vocab_pad, dim), bf16),
                pltpu.VMEM((width, dim), bf16),
                pltpu.VMEM((width, dim), bf16),
                pltpu.VMEM((2 * block, vocab_pad), bf16),
                pltpu.VMEM((ring, HALVES, 2 * block, half_w), bf16),
                pltpu.VMEM((HALVES, block, half_w), bf16),
                pltpu.VMEM((HALVES, block, half_w), bf16),
                pltpu.VMEM((2, HALVES, block, half_w), bf16),
                pltpu.VMEM((2, HALVES, block, half_w), f32),
                pltpu.VMEM((HALVES, block, half_w), f32),
                pltpu.VMEM((ring, HALVES, block, half_w), f32),
                pltpu.VMEM((ring - 1, HALVES, block, half_w), f32),
                pltpu.VMEM((2, HALVES, block, half_w), f32),
                dma((dim // min(512, half_w),)),
                dma((2,)),
                dma((HALVES,)), dma((ring, HALVES)),
                dma((2, HALVES)), dma((ring - 1, HALVES)),
                dma((ring, HALVES)), dma((ring, HALVES)),
                dma((ring, HALVES)), dma((ring, HALVES)),
                dma((HALVES,)), dma((ring, HALVES)),
                dma((2, HALVES)), dma((ring - 1, HALVES)),
                pltpu.SemaphoreType.REGULAR,
                pltpu.SemaphoreType.REGULAR,
            ],
            compiler_params=pltpu.CompilerParams(
                collective_id=0, has_side_effects=True, vmem_limit_bytes=VMEM_BYTES
            ),
        )(token_ids.reshape(tokens, 1), table_shard, norm_gain.reshape(1, dim), w_in_shard.T, w_out_shard)

    return jax.shard_map(
        device_step,
        mesh=mesh,
        in_specs=(P("dp"), P("tp", None), P(), P(None, "tp"), P("tp", None)),
        out_specs=P(("dp", "tp"), None),
        check_vma=False,
    )
```

```python
import functools

import jax
import jax.numpy as jnp
from jax import lax
from jax.experimental import pallas as pl
from jax.experimental.pallas import tpu as pltpu
from jax.sharding import PartitionSpec as P

MESH = pl.DeviceIdType.MESH
RMS_EPS = 1e-6
CORES = 2
PIECES = 4
LAG = 2
VMEM_BYTES = 67043328


def block_kernel(
    group, ids_ref, table_hbm, gain_ref, w1_hbm, w2_hbm, out_ref,
    table, w1, w2, onehot, xa, x_own, p1send, r1send,
    ymine, ysend, ypart, r2recv, r2send,
    load_sem, w_sem, p1_ssem, p1_rsem, r1_ssem, r1_rsem,
    ag_ssem, ag_rsem, agp_ssem, agp_rsem, yp_ssem, yp_rsem, r2_ssem, r2_rsem,
    credit_ring, credit_core,
):
    ring = group // CORES
    me = lax.axis_index("tp")
    z, core = me // CORES, me % CORES
    step_dir = 1 - 2 * core
    nxt = lax.rem(z + step_dir + ring, ring) * CORES + core
    prv = lax.rem(z - step_dir + ring, ring) * CORES + core
    mate = z * CORES + (1 - core)

    block = out_ref.shape[0]
    piece_w = xa.shape[3]
    vocab = table_hbm.shape[0]
    vocab_pad = table.shape[0]
    tile_g = min(512, piece_w)
    tile_y = min(512, piece_w)
    tiles = piece_w * PIECES // tile_g

    def remote(src, dst, ssem, rsem, dev):
        return pltpu.make_async_remote_copy(
            src_ref=src, dst_ref=dst, send_sem=ssem, recv_sem=rsem,
            device_id={"tp": dev}, device_id_type=MESH,
        )

    def table_load(j):
        cols = pl.ds(j * tile_g, tile_g)
        return pltpu.make_async_copy(
            table_hbm.at[:, cols], table.at[pl.ds(0, vocab), cols], load_sem.at[j]
        )

    for j in range(tiles):
        table_load(j).start()

    barrier = pltpu.get_barrier_semaphore()
    for dev in (nxt, prv, mate):
        pl.semaphore_signal(barrier, inc=1, device_id={"tp": dev}, device_id_type=MESH)

    if vocab_pad > vocab:
        table[vocab:, :] = jnp.zeros((vocab_pad - vocab, table.shape[1]), table.dtype)
    pl.semaphore_wait(barrier, 3)

    def w1_load():
        return pltpu.make_async_copy(w1_hbm, w1, w_sem.at[0])

    def w2_load():
        return pltpu.make_async_copy(w2_hbm, w2, w_sem.at[1])

    def p1_copy(t, h):
        return remote(
            p1send.at[h], xa.at[t, h, pl.ds(block, block)],
            p1_ssem.at[h], p1_rsem.at[t, h], mate,
        )

    def r1_copy(t, h):
        return remote(
            r1send.at[t % 2, h], xa.at[t, h, pl.ds(0, block)],
            r1_ssem.at[t % 2, h], r1_rsem.at[t, h], nxt,
        )

    def chip_back(s):
        return lax.rem(z - step_dir * s + 2 * ring, ring)

    def chip_ahead(s):
        return lax.rem(z + step_dir * s + 2 * ring, ring)

    def fill_onehot(t):
        for row, chip, c in ((0, chip_back(1 + t), core), (block, chip_ahead(1 + t), 1 - core)):
            line = ids_ref[pl.ds(chip, 1), :].astype(jnp.float32)
            lanes = lax.broadcasted_iota(jnp.int32, (block, CORES * block), 1)
            rows = lax.broadcasted_iota(jnp.int32, (block, CORES * block), 0)
            mine = jnp.where(lanes == rows + c * block, line, 0.0)
            column = jnp.sum(mine, axis=1, keepdims=True).astype(jnp.int32)
            local = column - me * vocab
            slots = lax.broadcasted_iota(jnp.int32, (block, vocab_pad), 1)
            hit = jnp.where((slots == local) & (slots < vocab), 1.0, 0.0)
            onehot[pl.ds(row, block), :] = hit.astype(jnp.bfloat16)

    def gather_piece(t, h):
        for j in range(piece_w // tile_g):
            g = h * (piece_w // tile_g) + j

            @pl.when(t == 0)
            def _():
                table_load(g).wait()

            rows = jnp.dot(
                onehot[...], table[:, g * tile_g:(g + 1) * tile_g],
                preferred_element_type=jnp.float32,
            ).astype(jnp.bfloat16)
            cols = slice(j * tile_g, (j + 1) * tile_g)
            x_own[h, :, cols] = rows[:block]
            p1send[h, :, cols] = rows[block:]

    def ring1_piece(t, h):
        p1_copy(t, h).wait_recv()

        @pl.when(t >= 2)
        def _():
            r1_copy(t - 2, h).wait_send()

        r1send[t % 2, h] = x_own[h] + xa[t, h, block:]

        @pl.when(t >= 1)
        def _():
            r1_copy(t - 1, h).wait_recv()
            r1send[t % 2, h] = r1send[t % 2, h] + xa[t - 1, h, :block]

        r1_copy(t, h).start()

    def rows_step(t, carry):
        fill_onehot(t)

        @pl.when(t == 1)
        def _():
            w1_load().start()
            w2_load().start()

        for h in range(PIECES):
            @pl.when(t >= 1)
            def _():
                p1_copy(t - 1, h).wait_send()

            gather_piece(t, h)
            p1_copy(t, h).start()
            if h < LAG:
                @pl.when(t >= 1)
                def _():
                    ring1_piece(t - 1, h + PIECES - LAG)
            else:
                @pl.when(t < ring - 1)
                def _():
                    ring1_piece(t, h - LAG)
        return carry

    lax.fori_loop(0, ring, rows_step, 0)

    last = ring - 1
    for h in range(PIECES):
        p1_copy(last, h).wait_recv()
        r1_copy(last - 1, h).wait_recv()
        x_own[h] = x_own[h] + xa[last, h, block:] + xa[last - 1, h, :block]
    pl.semaphore_signal(credit_ring, inc=1, device_id={"tp": prv}, device_id_type=MESH)
    pl.semaphore_signal(credit_core, inc=1, device_id={"tp": mate}, device_id_type=MESH)

    def ag_copy(s, h):
        return remote(
            xa.at[s, h, pl.ds(0, block)], xa.at[s + 1, h, pl.ds(0, block)],
            ag_ssem.at[s, h], ag_rsem.at[s, h], nxt,
        )

    def agp_copy(s, h):
        return remote(
            xa.at[s, h, pl.ds(0, block)], xa.at[s, h, pl.ds(block, block)],
            agp_ssem.at[s, h], agp_rsem.at[s, h], mate,
        )

    def yp_copy(s, h):
        return remote(
            ysend.at[h], ypart.at[s, h],
            yp_ssem.at[h], yp_rsem.at[s, h], mate,
        )

    def r2_copy(s, h):
        return remote(
            r2send.at[s % 2, h], r2recv.at[s - 1, h],
            r2_ssem.at[s % 2, h], r2_rsem.at[s - 1, h], nxt,
        )

    total = jnp.zeros((block, 1), jnp.float32)
    for h in range(PIECES):
        xf = x_own[h].astype(jnp.float32)
        total = total + jnp.sum(xf * xf, axis=-1, keepdims=True)
    inv_rms = lax.rsqrt(total / (piece_w * PIECES) + RMS_EPS)
    gain = gain_ref[...].astype(jnp.float32)
    lines = piece_w // gain.shape[1]
    pl.semaphore_wait(credit_ring, 1)
    pl.semaphore_wait(credit_core, 1)
    for h in range(PIECES):
        for k in range(lines):
            cols = slice(k * gain.shape[1], (k + 1) * gain.shape[1])
            g = gain[h * lines + k:h * lines + k + 1, :]
            xf = x_own[h, :, cols].astype(jnp.float32)
            xa[0, h, :block, cols] = (xf * inv_rms * g).astype(jnp.bfloat16)
        ag_copy(0, h).start()
        agp_copy(0, h).start()
    w1_load().wait()
    w2_load().wait()

    def combine(s, h):
        yp_copy(s, h).wait_recv()

        @pl.when(s >= 3)
        def _():
            r2_copy(s - 2, h).wait_send()

        r2send[s % 2, h] = ymine[1, h] + ypart[s, h]

        @pl.when(s >= 2)
        def _():
            r2_copy(s - 1, h).wait_recv()
            r2send[s % 2, h] = r2send[s % 2, h] + r2recv[s - 2, h]

        r2_copy(s, h).start()

    def mlp_step(s, carry):
        for h in range(PIECES):
            @pl.when(s >= 1)
            def _():
                ag_copy(s - 1, h).wait_recv()

            @pl.when((s >= 1) & (s < ring - 1))
            def _():
                ag_copy(s, h).start()

            @pl.when(s >= 1)
            def _():
                agp_copy(s, h).start()

        acc = None
        for h in range(PIECES):
            agp_copy(s, h).wait_recv()
            part = lax.dot_general(
                xa[s, h], w1[:, h * piece_w:(h + 1) * piece_w], (((1,), (1,)), ((), ())),
                preferred_element_type=jnp.float32,
            )
            acc = part if acc is None else acc + part
        u = acc.astype(jnp.bfloat16).astype(jnp.float32)
        act = jax.nn.gelu(u, approximate=True).astype(jnp.bfloat16)

        kept = jnp.minimum(s, 1)
        for h in range(PIECES):
            @pl.when(s >= 1)
            def _():
                yp_copy(s - 1, h).wait_send()

            for j in range(piece_w // tile_y):
                c0 = h * piece_w + j * tile_y
                y = jnp.dot(act, w2[:, c0:c0 + tile_y], preferred_element_type=jnp.float32)
                cols = slice(j * tile_y, (j + 1) * tile_y)
                ymine[kept, h, :, cols] = y[:block]
                ysend[h, :, cols] = y[block:]
            yp_copy(s, h).start()
            if h >= LAG:
                @pl.when(s >= 1)
                def _():
                    combine(s, h - LAG)

        for h in range(PIECES - LAG, PIECES):
            @pl.when(s >= 1)
            def _():
                combine(s, h)
        return carry

    lax.fori_loop(0, ring, mlp_step, 0)

    for h in range(PIECES):
        yp_copy(0, h).wait_recv()
        r2_copy(ring - 1, h).wait_recv()
        own = ymine[0, h] + ypart[0, h] + r2recv[ring - 2, h]
        out_ref[:, h * piece_w:(h + 1) * piece_w] = (
            x_own[h].astype(jnp.float32) + own
        ).astype(jnp.bfloat16)

    for h in range(PIECES):
        p1_copy(last, h).wait_send()
        yp_copy(last, h).wait_send()
        for t in (ring - 2, ring - 1):
            r1_copy(t - 1, h).wait_send()
            r2_copy(t, h).wait_send()
        for s in range(ring):
            agp_copy(s, h).wait_send()
            if s < ring - 1:
                ag_copy(s, h).wait_send()


def solution(mesh):
    group = mesh.shape["tp"]
    ring = group // CORES

    def device_step(token_ids, table_shard, norm_gain, w_in_shard, w_out_shard):
        tokens = token_ids.shape[0]
        vocab, dim = table_shard.shape
        width = w_in_shard.shape[1]
        block, piece_w = tokens // group, dim // PIECES
        vocab_pad = -(-vocab // 256) * 256
        bf16, f32 = jnp.bfloat16, jnp.float32
        dma = pltpu.SemaphoreType.DMA
        vmem = pl.BlockSpec(memory_space=pltpu.VMEM)
        hbm = pl.BlockSpec(memory_space=pl.ANY)
        return pl.pallas_call(
            functools.partial(block_kernel, group),
            name="lookup_mlp",
            out_shape=jax.ShapeDtypeStruct((block, dim), bf16),
            in_specs=[vmem, hbm, vmem, hbm, hbm],
            out_specs=vmem,
            scratch_shapes=[
                pltpu.VMEM((vocab_pad, dim), bf16),
                pltpu.VMEM((width, dim), bf16),
                pltpu.VMEM((width, dim), bf16),
                pltpu.VMEM((2 * block, vocab_pad), bf16),
                pltpu.VMEM((ring, PIECES, 2 * block, piece_w), bf16),
                pltpu.VMEM((PIECES, block, piece_w), bf16),
                pltpu.VMEM((PIECES, block, piece_w), bf16),
                pltpu.VMEM((2, PIECES, block, piece_w), bf16),
                pltpu.VMEM((2, PIECES, block, piece_w), f32),
                pltpu.VMEM((PIECES, block, piece_w), f32),
                pltpu.VMEM((ring, PIECES, block, piece_w), f32),
                pltpu.VMEM((ring - 1, PIECES, block, piece_w), f32),
                pltpu.VMEM((2, PIECES, block, piece_w), f32),
                dma((dim // min(512, piece_w),)),
                dma((2,)),
                dma((PIECES,)), dma((ring, PIECES)),
                dma((2, PIECES)), dma((ring - 1, PIECES)),
                dma((ring, PIECES)), dma((ring, PIECES)),
                dma((ring, PIECES)), dma((ring, PIECES)),
                dma((PIECES,)), dma((ring, PIECES)),
                dma((2, PIECES)), dma((ring - 1, PIECES)),
                pltpu.SemaphoreType.REGULAR,
                pltpu.SemaphoreType.REGULAR,
            ],
            compiler_params=pltpu.CompilerParams(
                collective_id=0, has_side_effects=True, vmem_limit_bytes=VMEM_BYTES
            ),
        )(
            token_ids.reshape(ring, CORES * block), table_shard, norm_gain.reshape(dim // 128, 128),
            w_in_shard.T, w_out_shard,
        )

    return jax.shard_map(
        device_step,
        mesh=mesh,
        in_specs=(P("dp"), P("tp", None), P(), P(None, "tp"), P("tp", None)),
        out_specs=P(("dp", "tp"), None),
        check_vma=False,
    )
```

```python
import functools

import jax
import jax.numpy as jnp
from jax import lax
from jax.experimental import pallas as pl
from jax.experimental.pallas import tpu as pltpu
from jax.sharding import PartitionSpec as P

MESH = pl.DeviceIdType.MESH
RMS_EPS = 1e-6
CORES = 2
PIECES = 4
LAG = 2
VMEM_BYTES = 67043328


def block_kernel(
    group, ids_hbm, table_hbm, gain_hbm, w1_hbm, w2_hbm, out_ref,
    ids_ref, gain_ref, table, w1, w2, onehot, xa, x_own, p1send, r1send,
    ymine, ysend, ypart, r2recv, r2send,
    load_sem, w_sem, p1_ssem, p1_rsem, r1_ssem, r1_rsem,
    ag_ssem, ag_rsem, agp_ssem, agp_rsem, yp_ssem, yp_rsem, r2_ssem, r2_rsem,
    credit_ring, credit_core, late_ring, late_core,
):
    ring = group // CORES
    me = lax.axis_index("tp")
    z, core = me // CORES, me % CORES
    step_dir = 1 - 2 * core
    nxt = lax.rem(z + step_dir + ring, ring) * CORES + core
    prv = lax.rem(z - step_dir + ring, ring) * CORES + core
    mate = z * CORES + (1 - core)

    block = out_ref.shape[0]
    piece_w = xa.shape[3]
    vocab = table_hbm.shape[0]
    vocab_pad = table.shape[0]
    tile_g = min(512, piece_w)
    tile_y = min(512, piece_w)
    tiles = piece_w * PIECES // tile_g

    def remote(src, dst, ssem, rsem, dev):
        return pltpu.make_async_remote_copy(
            src_ref=src, dst_ref=dst, send_sem=ssem, recv_sem=rsem,
            device_id={"tp": dev}, device_id_type=MESH,
        )

    def table_load(j):
        cols = pl.ds(j * tile_g, tile_g)
        return pltpu.make_async_copy(
            table_hbm.at[:, cols], table.at[pl.ds(0, vocab), cols], load_sem.at[j]
        )

    def signal(sem, dev):
        pl.semaphore_signal(sem, inc=1, device_id={"tp": dev}, device_id_type=MESH)

    barrier = pltpu.get_barrier_semaphore()
    for dev in (nxt, prv, mate):
        signal(barrier, dev)

    ids_load = pltpu.make_async_copy(ids_hbm, ids_ref, w_sem.at[2])
    gain_load = pltpu.make_async_copy(gain_hbm, gain_ref, w_sem.at[3])
    ids_load.start()
    for j in range(tiles):
        table_load(j).start()
    gain_load.start()

    if vocab_pad > vocab:
        table[vocab:, :] = jnp.zeros((vocab_pad - vocab, table.shape[1]), table.dtype)
    ids_load.wait()
    gain_load.wait()
    pl.semaphore_wait(barrier, 3)

    def w1_load():
        return pltpu.make_async_copy(w1_hbm, w1, w_sem.at[0])

    def w2_load():
        return pltpu.make_async_copy(w2_hbm, w2, w_sem.at[1])

    def p1_copy(t, h):
        return remote(
            p1send.at[h], xa.at[t, h, pl.ds(block, block)],
            p1_ssem.at[h], p1_rsem.at[t, h], mate,
        )

    def r1_copy(t, h):
        return remote(
            r1send.at[t % 2, h], xa.at[t, h, pl.ds(0, block)],
            r1_ssem.at[t % 2, h], r1_rsem.at[t, h], nxt,
        )

    def chip_back(s):
        return lax.rem(z - step_dir * s + 2 * ring, ring)

    def chip_ahead(s):
        return lax.rem(z + step_dir * s + 2 * ring, ring)

    def fill_onehot(t):
        for row, chip, c in ((0, chip_back(1 + t), core), (block, chip_ahead(1 + t), 1 - core)):
            line = ids_ref[pl.ds(chip, 1), :].astype(jnp.float32)
            lanes = lax.broadcasted_iota(jnp.int32, (block, CORES * block), 1)
            rows = lax.broadcasted_iota(jnp.int32, (block, CORES * block), 0)
            mine = jnp.where(lanes == rows + c * block, line, 0.0)
            column = jnp.sum(mine, axis=1, keepdims=True).astype(jnp.int32)
            local = column - me * vocab
            slots = lax.broadcasted_iota(jnp.int32, (block, vocab_pad), 1)
            hit = jnp.where(slots == local, 1.0, 0.0)
            onehot[pl.ds(row, block), :] = hit.astype(jnp.bfloat16)

    def gather_piece(t, h):
        for j in range(piece_w // tile_g):
            g = h * (piece_w // tile_g) + j

            @pl.when(t == 0)
            def _():
                table_load(g).wait()

            rows = jnp.dot(
                onehot[...], table[:, g * tile_g:(g + 1) * tile_g],
                preferred_element_type=jnp.float32,
            ).astype(jnp.bfloat16)
            cols = slice(j * tile_g, (j + 1) * tile_g)
            x_own[h, :, cols] = rows[:block]
            p1send[h, :, cols] = rows[block:]

    def ring1_piece(t, h):
        p1_copy(t, h).wait_recv()

        @pl.when(t >= 2)
        def _():
            r1_copy(t - 2, h).wait_send()

        @pl.when(t == 0)
        def _():
            r1send[t % 2, h] = x_own[h] + xa[t, h, block:]

        @pl.when(t >= 1)
        def _():
            r1_copy(t - 1, h).wait_recv()
            r1send[t % 2, h] = x_own[h] + xa[t, h, block:] + xa[t - 1, h, :block]

        r1_copy(t, h).start()

    def rows_step(t, carry):
        fill_onehot(t)

        @pl.when(t == 1)
        def _():
            w1_load().start()
            w2_load().start()

        for h in range(PIECES):
            @pl.when(t >= 1)
            def _():
                p1_copy(t - 1, h).wait_send()

            gather_piece(t, h)
            p1_copy(t, h).start()
            if h < LAG:
                @pl.when(t >= 1)
                def _():
                    ring1_piece(t - 1, h + PIECES - LAG)
            else:
                @pl.when(t < ring - 1)
                def _():
                    ring1_piece(t, h - LAG)
        return carry

    lax.fori_loop(0, ring, rows_step, 0)

    signal(credit_ring, prv)
    signal(credit_core, mate)
    last = ring - 1
    total = jnp.zeros((block, 1), jnp.float32)
    for h in range(PIECES):
        p1_copy(last, h).wait_recv()
        r1_copy(last - 1, h).wait_recv()
        x_own[h] = x_own[h] + xa[last, h, block:] + xa[last - 1, h, :block]
        xf = x_own[h].astype(jnp.float32)
        total = total + jnp.sum(xf * xf, axis=-1, keepdims=True)
    signal(late_ring, prv)
    signal(late_core, mate)

    def ag_copy(s, h):
        return remote(
            xa.at[s, h, pl.ds(0, block)], xa.at[s + 1, h, pl.ds(0, block)],
            ag_ssem.at[s, h], ag_rsem.at[s, h], nxt,
        )

    def agp_copy(s, h):
        return remote(
            xa.at[s, h, pl.ds(0, block)], xa.at[s, h, pl.ds(block, block)],
            agp_ssem.at[s, h], agp_rsem.at[s, h], mate,
        )

    def yp_copy(s, h):
        return remote(
            ysend.at[h], ypart.at[s, h],
            yp_ssem.at[h], yp_rsem.at[s, h], mate,
        )

    def r2_copy(s, h):
        return remote(
            r2send.at[s % 2, h], r2recv.at[s - 1, h],
            r2_ssem.at[s % 2, h], r2_rsem.at[s - 1, h], nxt,
        )

    inv_rms = lax.rsqrt(total / (piece_w * PIECES) + RMS_EPS)
    gain = gain_ref[...].astype(jnp.float32)
    lines = piece_w // gain.shape[1]
    pl.semaphore_wait(credit_ring, 1)
    pl.semaphore_wait(credit_core, 1)
    for h in range(PIECES):
        for k in range(lines):
            cols = slice(k * gain.shape[1], (k + 1) * gain.shape[1])
            g = gain[h * lines + k:h * lines + k + 1, :]
            xf = x_own[h, :, cols].astype(jnp.float32)
            xa[0, h, :block, cols] = (xf * inv_rms * g).astype(jnp.bfloat16)
        ag_copy(0, h).start()
        agp_copy(0, h).start()
    pl.semaphore_wait(late_ring, 1)
    pl.semaphore_wait(late_core, 1)
    w1_load().wait()
    w2_load().wait()

    def combine(s, h):
        yp_copy(s, h).wait_recv()

        @pl.when(s >= 3)
        def _():
            r2_copy(s - 2, h).wait_send()

        @pl.when(s == 1)
        def _():
            r2send[s % 2, h] = ymine[1, h] + ypart[s, h]

        @pl.when(s >= 2)
        def _():
            r2_copy(s - 1, h).wait_recv()
            r2send[s % 2, h] = ymine[1, h] + ypart[s, h] + r2recv[s - 2, h]

        r2_copy(s, h).start()

    def mlp_step(s, carry):
        acc = None
        for h in range(PIECES):
            agp_copy(s, h).wait_recv()
            part = lax.dot_general(
                xa[s, h], w1[:, h * piece_w:(h + 1) * piece_w], (((1,), (1,)), ((), ())),
                preferred_element_type=jnp.float32,
            )
            acc = part if acc is None else acc + part
        u = acc.astype(jnp.bfloat16).astype(jnp.float32)
        act = jax.nn.gelu(u, approximate=True).astype(jnp.bfloat16)

        kept = jnp.minimum(s, 1)
        for h in range(PIECES):
            @pl.when(s < ring - 1)
            def _():
                ag_copy(s, h).wait_recv()
                agp_copy(s + 1, h).start()

            @pl.when(s < ring - 2)
            def _():
                ag_copy(s + 1, h).start()

            @pl.when(s >= 1)
            def _():
                yp_copy(s - 1, h).wait_send()

            for j in range(piece_w // tile_y):
                c0 = h * piece_w + j * tile_y
                y = jnp.dot(act, w2[:, c0:c0 + tile_y], preferred_element_type=jnp.float32)
                cols = slice(j * tile_y, (j + 1) * tile_y)
                ymine[kept, h, :, cols] = y[:block]
                ysend[h, :, cols] = y[block:]
            yp_copy(s, h).start()
            if h >= LAG:
                @pl.when(s >= 1)
                def _():
                    combine(s, h - LAG)

        for h in range(PIECES - LAG, PIECES):
            @pl.when(s >= 1)
            def _():
                combine(s, h)
        return carry

    lax.fori_loop(0, ring, mlp_step, 0)

    for h in range(PIECES):
        yp_copy(0, h).wait_recv()
        r2_copy(ring - 1, h).wait_recv()
        own = ymine[0, h] + ypart[0, h] + r2recv[ring - 2, h]
        out_ref[:, h * piece_w:(h + 1) * piece_w] = (
            x_own[h].astype(jnp.float32) + own
        ).astype(jnp.bfloat16)

    for h in range(PIECES):
        p1_copy(last, h).wait_send()
        yp_copy(last, h).wait_send()
        for t in (ring - 2, ring - 1):
            r1_copy(t - 1, h).wait_send()
            r2_copy(t, h).wait_send()
        for s in range(ring):
            agp_copy(s, h).wait_send()
            if s < ring - 1:
                ag_copy(s, h).wait_send()


def solution(mesh):
    group = mesh.shape["tp"]
    ring = group // CORES

    def device_step(token_ids, table_shard, norm_gain, w_in_shard, w_out_shard):
        tokens = token_ids.shape[0]
        vocab, dim = table_shard.shape
        width = w_in_shard.shape[1]
        block, piece_w = tokens // group, dim // PIECES
        vocab_pad = -(-vocab // 256) * 256
        bf16, f32 = jnp.bfloat16, jnp.float32
        dma = pltpu.SemaphoreType.DMA
        vmem = pl.BlockSpec(memory_space=pltpu.VMEM)
        hbm = pl.BlockSpec(memory_space=pl.ANY)
        return pl.pallas_call(
            functools.partial(block_kernel, group),
            name="lookup_mlp",
            out_shape=jax.ShapeDtypeStruct((block, dim), bf16),
            in_specs=[hbm] * 5,
            out_specs=vmem,
            scratch_shapes=[
                pltpu.VMEM((ring, CORES * block), jnp.int32),
                pltpu.VMEM((dim // 128, 128), bf16),
                pltpu.VMEM((vocab_pad, dim), bf16),
                pltpu.VMEM((width, dim), bf16),
                pltpu.VMEM((width, dim), bf16),
                pltpu.VMEM((2 * block, vocab_pad), bf16),
                pltpu.VMEM((ring, PIECES, 2 * block, piece_w), bf16),
                pltpu.VMEM((PIECES, block, piece_w), bf16),
                pltpu.VMEM((PIECES, block, piece_w), bf16),
                pltpu.VMEM((2, PIECES, block, piece_w), bf16),
                pltpu.VMEM((2, PIECES, block, piece_w), f32),
                pltpu.VMEM((PIECES, block, piece_w), f32),
                pltpu.VMEM((ring, PIECES, block, piece_w), f32),
                pltpu.VMEM((ring - 1, PIECES, block, piece_w), f32),
                pltpu.VMEM((2, PIECES, block, piece_w), f32),
                dma((dim // min(512, piece_w),)),
                dma((4,)),
                dma((PIECES,)), dma((ring, PIECES)),
                dma((2, PIECES)), dma((ring - 1, PIECES)),
                dma((ring, PIECES)), dma((ring, PIECES)),
                dma((ring, PIECES)), dma((ring, PIECES)),
                dma((PIECES,)), dma((ring, PIECES)),
                dma((2, PIECES)), dma((ring - 1, PIECES)),
            ] + [pltpu.SemaphoreType.REGULAR] * 4,
            compiler_params=pltpu.CompilerParams(
                collective_id=0, has_side_effects=True, vmem_limit_bytes=VMEM_BYTES
            ),
        )(
            token_ids.reshape(ring, CORES * block), table_shard, norm_gain.reshape(dim // 128, 128),
            w_in_shard.T, w_out_shard,
        )

    return jax.shard_map(
        device_step,
        mesh=mesh,
        in_specs=(P("dp"), P("tp", None), P(), P(None, "tp"), P("tp", None)),
        out_specs=P(("dp", "tp"), None),
        check_vma=False,
    )
```

```python
import functools

import jax
import jax.numpy as jnp
from jax import lax
from jax.experimental import pallas as pl
from jax.experimental.pallas import tpu as pltpu
from jax.sharding import PartitionSpec as P

MESH = pl.DeviceIdType.MESH
RMS_EPS = 1e-6
CORES = 2
PIECES = 4
ROW_LAG = 1
LAG = 2
AHEAD = 3
VMEM_BYTES = 65536000


def block_kernel(
    group, ids_hbm, table_hbm, gain_hbm, w1_hbm, w2_hbm, out_ref,
    ids_ref, gain_ref, table, w1, w2, onehot, xa, x_own, p1send, r1send,
    ymine, ysend, ypart, r2recv, r2send,
    load_sem, w_sem, p1_ssem, p1_rsem, r1_ssem, r1_rsem,
    ag_ssem, ag_rsem, agp_ssem, agp_rsem, yp_ssem, yp_rsem, r2_ssem, r2_rsem,
    credit_ring, credit_core, late_ring, late_core,
):
    ring = group // CORES
    me = lax.axis_index("tp")
    z, core = me // CORES, me % CORES
    step_dir = 1 - 2 * core
    nxt = lax.rem(z + step_dir + ring, ring) * CORES + core
    prv = lax.rem(z - step_dir + ring, ring) * CORES + core
    mate = z * CORES + (1 - core)

    block = out_ref.shape[0]
    piece_w = xa.shape[3]
    vocab = table_hbm.shape[0]
    vocab_pad = table.shape[0]
    tile_g = min(512, piece_w)
    tile_y = min(512, piece_w)
    tiles = piece_w * PIECES // tile_g

    def remote(src, dst, ssem, rsem, dev):
        return pltpu.make_async_remote_copy(
            src_ref=src, dst_ref=dst, send_sem=ssem, recv_sem=rsem,
            device_id={"tp": dev}, device_id_type=MESH,
        )

    def table_load(j):
        cols = pl.ds(j * tile_g, tile_g)
        return pltpu.make_async_copy(
            table_hbm.at[:, cols], table.at[pl.ds(0, vocab), cols], load_sem.at[j]
        )

    def signal(sem, dev):
        pl.semaphore_signal(sem, inc=1, device_id={"tp": dev}, device_id_type=MESH)

    barrier = pltpu.get_barrier_semaphore()
    for dev in (nxt, prv, mate):
        signal(barrier, dev)

    ids_load = pltpu.make_async_copy(ids_hbm, ids_ref, w_sem.at[2])
    gain_load = pltpu.make_async_copy(gain_hbm, gain_ref, w_sem.at[3])
    ids_load.start()
    for j in range(AHEAD):
        table_load(j).start()
    gain_load.start()

    if vocab_pad > vocab:
        table[vocab:, :] = jnp.zeros((vocab_pad - vocab, table.shape[1]), table.dtype)
    ids_load.wait()
    gain_load.wait()
    pl.semaphore_wait(barrier, 3)

    def w1_load():
        return pltpu.make_async_copy(w1_hbm, w1, w_sem.at[0])

    def w2_load():
        return pltpu.make_async_copy(w2_hbm, w2, w_sem.at[1])

    def p1_copy(t, h):
        return remote(
            p1send.at[h], xa.at[t, h, pl.ds(block, block)],
            p1_ssem.at[h], p1_rsem.at[t, h], mate,
        )

    def r1_copy(t, h):
        return remote(
            r1send.at[t % 2, h], xa.at[t, h, pl.ds(0, block)],
            r1_ssem.at[t % 2, h], r1_rsem.at[t, h], nxt,
        )

    def chip_back(s):
        return lax.rem(z - step_dir * s + 2 * ring, ring)

    def chip_ahead(s):
        return lax.rem(z + step_dir * s + 2 * ring, ring)

    def fill_onehot(t):
        for row, chip, c in ((0, chip_back(1 + t), core), (block, chip_ahead(1 + t), 1 - core)):
            line = ids_ref[pl.ds(chip, 1), :].astype(jnp.float32)
            lanes = lax.broadcasted_iota(jnp.int32, (block, CORES * block), 1)
            rows = lax.broadcasted_iota(jnp.int32, (block, CORES * block), 0)
            mine = jnp.where(lanes == rows + c * block, line, 0.0)
            column = jnp.sum(mine, axis=1, keepdims=True).astype(jnp.int32)
            local = column - me * vocab
            slots = lax.broadcasted_iota(jnp.int32, (block, vocab_pad), 1)
            hit = jnp.where(slots == local, 1.0, 0.0)
            onehot[pl.ds(row, block), :] = hit.astype(jnp.bfloat16)

    def gather_piece(t, h):
        for j in range(piece_w // tile_g):
            g = h * (piece_w // tile_g) + j

            @pl.when(t == 0)
            def _():
                table_load(g).wait()
                if g + AHEAD < tiles:
                    table_load(g + AHEAD).start()

            rows = jnp.dot(
                onehot[...], table[:, g * tile_g:(g + 1) * tile_g],
                preferred_element_type=jnp.float32,
            ).astype(jnp.bfloat16)
            cols = slice(j * tile_g, (j + 1) * tile_g)
            x_own[h, :, cols] = rows[:block]
            p1send[h, :, cols] = rows[block:]

    def ring1_piece(t, h):
        p1_copy(t, h).wait_recv()

        @pl.when(t >= 2)
        def _():
            r1_copy(t - 2, h).wait_send()

        @pl.when(t == 0)
        def _():
            r1send[t % 2, h] = x_own[h] + xa[t, h, block:]

        @pl.when(t >= 1)
        def _():
            r1_copy(t - 1, h).wait_recv()
            r1send[t % 2, h] = x_own[h] + xa[t, h, block:] + xa[t - 1, h, :block]

        r1_copy(t, h).start()

    def rows_step(t, carry):
        fill_onehot(t)

        @pl.when(t == 1)
        def _():
            w1_load().start()
            w2_load().start()

        for h in range(PIECES):
            @pl.when(t >= 1)
            def _():
                p1_copy(t - 1, h).wait_send()

            gather_piece(t, h)
            p1_copy(t, h).start()
            if h < ROW_LAG:
                @pl.when(t >= 1)
                def _():
                    ring1_piece(t - 1, h + PIECES - ROW_LAG)
            else:
                @pl.when(t < ring - 1)
                def _():
                    ring1_piece(t, h - ROW_LAG)
        return carry

    lax.fori_loop(0, ring, rows_step, 0)

    signal(credit_ring, prv)
    signal(credit_core, mate)
    last = ring - 1
    total = jnp.zeros((block, 1), jnp.float32)
    for h in range(PIECES):
        p1_copy(last, h).wait_recv()
        r1_copy(last - 1, h).wait_recv()
        x_own[h] = x_own[h] + xa[last, h, block:] + xa[last - 1, h, :block]
        xf = x_own[h].astype(jnp.float32)
        total = total + jnp.sum(xf * xf, axis=-1, keepdims=True)
    signal(late_ring, prv)
    signal(late_core, mate)

    def ag_copy(s, h):
        return remote(
            xa.at[s, h, pl.ds(0, block)], xa.at[s + 1, h, pl.ds(0, block)],
            ag_ssem.at[s, h], ag_rsem.at[s, h], nxt,
        )

    def agp_copy(s, h):
        return remote(
            xa.at[s, h, pl.ds(0, block)], xa.at[s, h, pl.ds(block, block)],
            agp_ssem.at[s, h], agp_rsem.at[s, h], mate,
        )

    def yp_copy(s, h):
        return remote(
            ysend.at[h], ypart.at[s, h],
            yp_ssem.at[h], yp_rsem.at[s, h], mate,
        )

    def r2_copy(s, h):
        return remote(
            r2send.at[s % 2, h], r2recv.at[s - 1, h],
            r2_ssem.at[s % 2, h], r2_rsem.at[s - 1, h], nxt,
        )

    inv_rms = lax.rsqrt(total / (piece_w * PIECES) + RMS_EPS)
    gain = gain_ref[...].astype(jnp.float32)
    lines = piece_w // gain.shape[1]
    pl.semaphore_wait(credit_ring, 1)
    pl.semaphore_wait(credit_core, 1)
    for h in range(PIECES):
        for k in range(lines):
            cols = slice(k * gain.shape[1], (k + 1) * gain.shape[1])
            g = gain[h * lines + k:h * lines + k + 1, :]
            xf = x_own[h, :, cols].astype(jnp.float32)
            xa[0, h, :block, cols] = (xf * inv_rms * g).astype(jnp.bfloat16)
        ag_copy(0, h).start()
        agp_copy(0, h).start()
    pl.semaphore_wait(late_ring, 1)
    pl.semaphore_wait(late_core, 1)
    w1_load().wait()
    w2_load().wait()

    def combine(s, h):
        yp_copy(s, h).wait_recv()

        @pl.when(s >= 3)
        def _():
            r2_copy(s - 2, h).wait_send()

        @pl.when(s == 1)
        def _():
            r2send[s % 2, h] = ymine[1, h] + ypart[s, h]

        @pl.when(s >= 2)
        def _():
            r2_copy(s - 1, h).wait_recv()
            r2send[s % 2, h] = ymine[1, h] + ypart[s, h] + r2recv[s - 2, h]

        r2_copy(s, h).start()

    def mlp_step(s, carry):
        acc = None
        for h in range(PIECES):
            agp_copy(s, h).wait_recv()
            part = lax.dot_general(
                xa[s, h], w1[:, h * piece_w:(h + 1) * piece_w], (((1,), (1,)), ((), ())),
                preferred_element_type=jnp.float32,
            )
            acc = part if acc is None else acc + part
        u = acc.astype(jnp.bfloat16).astype(jnp.float32)
        act = jax.nn.gelu(u, approximate=True).astype(jnp.bfloat16)

        kept = jnp.minimum(s, 1)
        for h in range(PIECES):
            @pl.when(s < ring - 1)
            def _():
                ag_copy(s, h).wait_recv()
                agp_copy(s + 1, h).start()

            @pl.when(s < ring - 2)
            def _():
                ag_copy(s + 1, h).start()

            @pl.when(s >= 1)
            def _():
                yp_copy(s - 1, h).wait_send()

            for j in range(piece_w // tile_y):
                c0 = h * piece_w + j * tile_y
                y = jnp.dot(act, w2[:, c0:c0 + tile_y], preferred_element_type=jnp.float32)
                cols = slice(j * tile_y, (j + 1) * tile_y)
                ymine[kept, h, :, cols] = y[:block]
                ysend[h, :, cols] = y[block:]
            yp_copy(s, h).start()
            if h >= LAG:
                @pl.when(s >= 1)
                def _():
                    combine(s, h - LAG)

        for h in range(PIECES - LAG, PIECES):
            @pl.when(s >= 1)
            def _():
                combine(s, h)
        return carry

    lax.fori_loop(0, ring, mlp_step, 0)

    for h in range(PIECES):
        yp_copy(0, h).wait_recv()
        r2_copy(ring - 1, h).wait_recv()
        own = ymine[0, h] + ypart[0, h] + r2recv[ring - 2, h]
        out_ref[:, h * piece_w:(h + 1) * piece_w] = (
            x_own[h].astype(jnp.float32) + own
        ).astype(jnp.bfloat16)

    for h in range(PIECES):
        p1_copy(last, h).wait_send()
        yp_copy(last, h).wait_send()
        for t in (ring - 2, ring - 1):
            r1_copy(t - 1, h).wait_send()
            r2_copy(t, h).wait_send()
        for s in range(ring):
            agp_copy(s, h).wait_send()
            if s < ring - 1:
                ag_copy(s, h).wait_send()


def solution(mesh):
    group = mesh.shape["tp"]
    ring = group // CORES

    def device_step(token_ids, table_shard, norm_gain, w_in_shard, w_out_shard):
        tokens = token_ids.shape[0]
        vocab, dim = table_shard.shape
        width = w_in_shard.shape[1]
        block, piece_w = tokens // group, dim // PIECES
        vocab_pad = -(-vocab // 256) * 256
        bf16, f32 = jnp.bfloat16, jnp.float32
        dma = pltpu.SemaphoreType.DMA
        vmem = pl.BlockSpec(memory_space=pltpu.VMEM)
        hbm = pl.BlockSpec(memory_space=pl.ANY)
        return pl.pallas_call(
            functools.partial(block_kernel, group),
            name="lookup_mlp",
            out_shape=pltpu.VMEM((block, dim), bf16),
            in_specs=[hbm] * 5,
            out_specs=vmem,
            scratch_shapes=[
                pltpu.VMEM((ring, CORES * block), jnp.int32),
                pltpu.VMEM((dim // 128, 128), bf16),
                pltpu.VMEM((vocab_pad, dim), bf16),
                pltpu.VMEM((width, dim), bf16),
                pltpu.VMEM((width, dim), bf16),
                pltpu.VMEM((2 * block, vocab_pad), bf16),
                pltpu.VMEM((ring, PIECES, 2 * block, piece_w), bf16),
                pltpu.VMEM((PIECES, block, piece_w), bf16),
                pltpu.VMEM((PIECES, block, piece_w), bf16),
                pltpu.VMEM((2, PIECES, block, piece_w), bf16),
                pltpu.VMEM((2, PIECES, block, piece_w), f32),
                pltpu.VMEM((PIECES, block, piece_w), f32),
                pltpu.VMEM((ring, PIECES, block, piece_w), f32),
                pltpu.VMEM((ring - 1, PIECES, block, piece_w), f32),
                pltpu.VMEM((2, PIECES, block, piece_w), f32),
                dma((dim // min(512, piece_w),)),
                dma((4,)),
                dma((PIECES,)), dma((ring, PIECES)),
                dma((2, PIECES)), dma((ring - 1, PIECES)),
                dma((ring, PIECES)), dma((ring, PIECES)),
                dma((ring, PIECES)), dma((ring, PIECES)),
                dma((PIECES,)), dma((ring, PIECES)),
                dma((2, PIECES)), dma((ring - 1, PIECES)),
            ] + [pltpu.SemaphoreType.REGULAR] * 4,
            compiler_params=pltpu.CompilerParams(
                collective_id=0, has_side_effects=True, vmem_limit_bytes=VMEM_BYTES
            ),
        )(
            token_ids.reshape(ring, CORES * block), table_shard, norm_gain.reshape(dim // 128, 128),
            w_in_shard.T, w_out_shard,
        )

    return jax.shard_map(
        device_step,
        mesh=mesh,
        in_specs=(P("dp"), P("tp", None), P(), P(None, "tp"), P("tp", None)),
        out_specs=P(("dp", "tp"), None),
        check_vma=False,
    )
```

```python
import functools

import jax
import jax.numpy as jnp
from jax import lax
from jax.experimental import pallas as pl
from jax.experimental.pallas import tpu as pltpu
from jax.sharding import PartitionSpec as P

MESH = pl.DeviceIdType.MESH
RMS_EPS = 1e-6
CORES = 2
PIECES = 4
ROW_LAG = 1
LAG = 2
AHEAD = 3
VMEM_BYTES = 65536000


def block_kernel(
    group, ids_hbm, table_hbm, gain_hbm, w1_hbm, w2_hbm, out_ref,
    ids_ref, gain_ref, table, w1, w2, onehot, xa, xn, x_own, p1send, r1send,
    ymine, ysend, ypart, r2recv, r2send,
    load_sem, w_sem, p1_ssem, p1_rsem, r1_ssem, r1_rsem,
    ag_ssem, ag_rsem, agp_ssem, agp_rsem, yp_ssem, yp_rsem, r2_ssem, r2_rsem,
    credit_ring, credit_core, late_ring, late_core,
):
    ring = group // CORES
    me = lax.axis_index("tp")
    z, core = me // CORES, me % CORES
    step_dir = 1 - 2 * core
    nxt = lax.rem(z + step_dir + ring, ring) * CORES + core
    prv = lax.rem(z - step_dir + ring, ring) * CORES + core
    mate = z * CORES + (1 - core)

    block = out_ref.shape[0]
    piece_w = xa.shape[3]
    vocab = table_hbm.shape[0]
    vocab_pad = table.shape[0]
    tile_g = min(512, piece_w)
    tile_y = min(512, piece_w)
    tiles = piece_w * PIECES // tile_g

    def remote(src, dst, ssem, rsem, dev):
        return pltpu.make_async_remote_copy(
            src_ref=src, dst_ref=dst, send_sem=ssem, recv_sem=rsem,
            device_id={"tp": dev}, device_id_type=MESH,
        )

    def table_load(j):
        cols = pl.ds(j * tile_g, tile_g)
        return pltpu.make_async_copy(
            table_hbm.at[:, cols], table.at[pl.ds(0, vocab), cols], load_sem.at[j]
        )

    def signal(sem, dev):
        pl.semaphore_signal(sem, inc=1, device_id={"tp": dev}, device_id_type=MESH)

    barrier = pltpu.get_barrier_semaphore()
    for dev in (nxt, prv, mate):
        signal(barrier, dev)

    ids_load = pltpu.make_async_copy(ids_hbm, ids_ref, w_sem.at[2])
    gain_load = pltpu.make_async_copy(gain_hbm, gain_ref, w_sem.at[3])
    ids_load.start()
    for j in range(AHEAD):
        table_load(j).start()
    gain_load.start()

    if vocab_pad > vocab:
        table[vocab:, :] = jnp.zeros((vocab_pad - vocab, table.shape[1]), table.dtype)
    ids_load.wait()
    gain_load.wait()
    pl.semaphore_wait(barrier, 3)

    def w1_load():
        return pltpu.make_async_copy(w1_hbm, w1, w_sem.at[0])

    def w2_load():
        return pltpu.make_async_copy(w2_hbm, w2, w_sem.at[1])

    def p1_copy(t, h):
        return remote(
            p1send.at[h], xa.at[t, h, pl.ds(block, block)],
            p1_ssem.at[h], p1_rsem.at[t, h], mate,
        )

    def r1_copy(t, h):
        return remote(
            r1send.at[t % 2, h], xa.at[t, h, pl.ds(0, block)],
            r1_ssem.at[t % 2, h], r1_rsem.at[t, h], nxt,
        )

    def chip_back(s):
        return lax.rem(z - step_dir * s + 2 * ring, ring)

    def chip_ahead(s):
        return lax.rem(z + step_dir * s + 2 * ring, ring)

    def fill_onehot(t):
        for row, chip, c in ((0, chip_back(1 + t), core), (block, chip_ahead(1 + t), 1 - core)):
            line = ids_ref[pl.ds(chip, 1), :].astype(jnp.float32)
            lanes = lax.broadcasted_iota(jnp.int32, (block, CORES * block), 1)
            rows = lax.broadcasted_iota(jnp.int32, (block, CORES * block), 0)
            mine = jnp.where(lanes == rows + c * block, line, 0.0)
            column = jnp.sum(mine, axis=1, keepdims=True).astype(jnp.int32)
            local = column - me * vocab
            slots = lax.broadcasted_iota(jnp.int32, (block, vocab_pad), 1)
            hit = jnp.where(slots == local, 1.0, 0.0)
            onehot[pl.ds(row, block), :] = hit.astype(jnp.bfloat16)

    def gather_piece(t, h):
        for j in range(piece_w // tile_g):
            g = h * (piece_w // tile_g) + j

            @pl.when(t == 0)
            def _():
                table_load(g).wait()
                if g + AHEAD < tiles:
                    table_load(g + AHEAD).start()

            rows = jnp.dot(
                onehot[...], table[:, g * tile_g:(g + 1) * tile_g],
                preferred_element_type=jnp.float32,
            ).astype(jnp.bfloat16)
            cols = slice(j * tile_g, (j + 1) * tile_g)
            x_own[h, :, cols] = rows[:block]
            p1send[h, :, cols] = rows[block:]

    def ring1_piece(t, h):
        p1_copy(t, h).wait_recv()

        @pl.when(t >= 2)
        def _():
            r1_copy(t - 2, h).wait_send()

        @pl.when(t == 0)
        def _():
            r1send[t % 2, h] = x_own[h] + xa[t, h, block:]

        @pl.when(t >= 1)
        def _():
            r1_copy(t - 1, h).wait_recv()
            r1send[t % 2, h] = x_own[h] + xa[t, h, block:] + xa[t - 1, h, :block]

        r1_copy(t, h).start()

    def ag_copy(s, h):
        return remote(
            xa.at[s, h, pl.ds(0, block)], xa.at[s + 1, h, pl.ds(0, block)],
            ag_ssem.at[s, h], ag_rsem.at[s, h], nxt,
        )

    def agp_copy(s, h):
        return remote(
            xa.at[s, h, pl.ds(0, block)], xa.at[s, h, pl.ds(block, block)],
            agp_ssem.at[s, h], agp_rsem.at[s, h], mate,
        )

    last = ring - 1

    def row_piece(t, h):
        @pl.when(t < last)
        def _():
            ring1_piece(t, h)

        @pl.when(t == last)
        def _():
            p1_copy(last, h).wait_recv()
            r1_copy(last - 1, h).wait_recv()
            xa[0, h, :block] = x_own[h] + xa[last, h, block:] + xa[last - 1, h, :block]
            if h == 0:
                pl.semaphore_wait(credit_ring, 1)
                pl.semaphore_wait(credit_core, 1)
            ag_copy(0, h).start()
            agp_copy(0, h).start()

    def rows_step(t, carry):
        fill_onehot(t)

        @pl.when(t == last)
        def _():
            signal(credit_ring, prv)
            signal(credit_core, mate)

        @pl.when(t == 1)
        def _():
            w1_load().start()
            w2_load().start()

        for h in range(PIECES):
            @pl.when(t >= 1)
            def _():
                p1_copy(t - 1, h).wait_send()

            gather_piece(t, h)
            p1_copy(t, h).start()
            if h < ROW_LAG:
                @pl.when(t >= 1)
                def _():
                    ring1_piece(t - 1, h + PIECES - ROW_LAG)
            else:
                row_piece(t, h - ROW_LAG)
        return carry

    lax.fori_loop(0, ring, rows_step, 0)

    for h in range(PIECES - ROW_LAG, PIECES):
        row_piece(last, h)
    signal(late_ring, prv)
    signal(late_core, mate)

    def yp_copy(s, h):
        return remote(
            ysend.at[h], ypart.at[s, h],
            yp_ssem.at[h], yp_rsem.at[s, h], mate,
        )

    def r2_copy(s, h):
        return remote(
            r2send.at[s % 2, h], r2recv.at[s - 1, h],
            r2_ssem.at[s % 2, h], r2_rsem.at[s - 1, h], nxt,
        )

    gain = gain_ref[...].astype(jnp.float32)
    lane_w = gain.shape[1]
    tiles_n = [(h, k) for h in range(PIECES) for k in range(piece_w // lane_w)]

    def normalize(s):
        squares = jnp.zeros((2 * block, lane_w), jnp.float32)
        for h, k in tiles_n:
            xf = xa[s, h, :, k * lane_w:(k + 1) * lane_w].astype(jnp.float32)
            squares = squares + xf * xf
        mean = jnp.sum(squares, axis=-1, keepdims=True) / (piece_w * PIECES)
        inv_rms = lax.rsqrt(mean + RMS_EPS)
        for line, (h, k) in enumerate(tiles_n):
            cols = slice(k * lane_w, (k + 1) * lane_w)
            xf = xa[s, h, :, cols].astype(jnp.float32)
            xn[h, :, cols] = (xf * inv_rms * gain[line:line + 1, :]).astype(jnp.bfloat16)

    w1_load().wait()
    w2_load().wait()

    def combine(s, h):
        yp_copy(s, h).wait_recv()

        @pl.when(s >= 3)
        def _():
            r2_copy(s - 2, h).wait_send()

        @pl.when(s == 1)
        def _():
            r2send[s % 2, h] = ymine[1, h] + ypart[s, h]

        @pl.when(s >= 2)
        def _():
            r2_copy(s - 1, h).wait_recv()
            r2send[s % 2, h] = ymine[1, h] + ypart[s, h] + r2recv[s - 2, h]

        r2_copy(s, h).start()

    def mlp_step(s, carry):
        @pl.when(s == 1)
        def _():
            pl.semaphore_wait(late_ring, 1)
            pl.semaphore_wait(late_core, 1)

        for h in range(PIECES):
            agp_copy(s, h).wait_recv()
        normalize(s)
        acc = None
        for h in range(PIECES):
            part = lax.dot_general(
                xn[h], w1[:, h * piece_w:(h + 1) * piece_w], (((1,), (1,)), ((), ())),
                preferred_element_type=jnp.float32,
            )
            acc = part if acc is None else acc + part
        u = acc.astype(jnp.bfloat16).astype(jnp.float32)
        act = jax.nn.gelu(u, approximate=True).astype(jnp.bfloat16)

        kept = jnp.minimum(s, 1)
        for h in range(PIECES):
            @pl.when(s < ring - 1)
            def _():
                ag_copy(s, h).wait_recv()
                agp_copy(s + 1, h).start()

            @pl.when(s < ring - 2)
            def _():
                ag_copy(s + 1, h).start()

            @pl.when(s >= 1)
            def _():
                yp_copy(s - 1, h).wait_send()

            for j in range(piece_w // tile_y):
                c0 = h * piece_w + j * tile_y
                y = jnp.dot(act, w2[:, c0:c0 + tile_y], preferred_element_type=jnp.float32)
                cols = slice(j * tile_y, (j + 1) * tile_y)
                ymine[kept, h, :, cols] = y[:block]
                ysend[h, :, cols] = y[block:]
            yp_copy(s, h).start()
            if h >= LAG:
                @pl.when(s >= 1)
                def _():
                    combine(s, h - LAG)

        for h in range(PIECES - LAG, PIECES):
            @pl.when(s >= 1)
            def _():
                combine(s, h)
        return carry

    lax.fori_loop(0, ring, mlp_step, 0)

    for h in range(PIECES):
        yp_copy(0, h).wait_recv()
        r2_copy(ring - 1, h).wait_recv()
        own = ymine[0, h] + ypart[0, h] + r2recv[ring - 2, h]
        out_ref[:, h * piece_w:(h + 1) * piece_w] = (
            xa[0, h, :block].astype(jnp.float32) + own
        ).astype(jnp.bfloat16)

    for h in range(PIECES):
        p1_copy(last, h).wait_send()
        yp_copy(last, h).wait_send()
        for t in (ring - 2, ring - 1):
            r1_copy(t - 1, h).wait_send()
            r2_copy(t, h).wait_send()
        for s in range(ring):
            agp_copy(s, h).wait_send()
            if s < ring - 1:
                ag_copy(s, h).wait_send()


def solution(mesh):
    group = mesh.shape["tp"]
    ring = group // CORES

    def device_step(token_ids, table_shard, norm_gain, w_in_shard, w_out_shard):
        tokens = token_ids.shape[0]
        vocab, dim = table_shard.shape
        width = w_in_shard.shape[1]
        block, piece_w = tokens // group, dim // PIECES
        vocab_pad = -(-vocab // 256) * 256
        bf16, f32 = jnp.bfloat16, jnp.float32
        dma = pltpu.SemaphoreType.DMA
        vmem = pl.BlockSpec(memory_space=pltpu.VMEM)
        hbm = pl.BlockSpec(memory_space=pl.ANY)
        return pl.pallas_call(
            functools.partial(block_kernel, group),
            name="lookup_mlp",
            out_shape=pltpu.VMEM((block, dim), bf16),
            in_specs=[hbm] * 5,
            out_specs=vmem,
            scratch_shapes=[
                pltpu.VMEM((ring, CORES * block), jnp.int32),
                pltpu.VMEM((dim // 128, 128), bf16),
                pltpu.VMEM((vocab_pad, dim), bf16),
                pltpu.VMEM((width, dim), bf16),
                pltpu.VMEM((width, dim), bf16),
                pltpu.VMEM((2 * block, vocab_pad), bf16),
                pltpu.VMEM((ring, PIECES, 2 * block, piece_w), bf16),
                pltpu.VMEM((PIECES, 2 * block, piece_w), bf16),
                pltpu.VMEM((PIECES, block, piece_w), bf16),
                pltpu.VMEM((PIECES, block, piece_w), bf16),
                pltpu.VMEM((2, PIECES, block, piece_w), bf16),
                pltpu.VMEM((2, PIECES, block, piece_w), f32),
                pltpu.VMEM((PIECES, block, piece_w), f32),
                pltpu.VMEM((ring, PIECES, block, piece_w), f32),
                pltpu.VMEM((ring - 1, PIECES, block, piece_w), f32),
                pltpu.VMEM((2, PIECES, block, piece_w), f32),
                dma((dim // min(512, piece_w),)),
                dma((4,)),
                dma((PIECES,)), dma((ring, PIECES)),
                dma((2, PIECES)), dma((ring - 1, PIECES)),
                dma((ring, PIECES)), dma((ring, PIECES)),
                dma((ring, PIECES)), dma((ring, PIECES)),
                dma((PIECES,)), dma((ring, PIECES)),
                dma((2, PIECES)), dma((ring - 1, PIECES)),
            ] + [pltpu.SemaphoreType.REGULAR] * 4,
            compiler_params=pltpu.CompilerParams(
                collective_id=0, has_side_effects=True, vmem_limit_bytes=VMEM_BYTES
            ),
        )(
            token_ids.reshape(ring, CORES * block), table_shard, norm_gain.reshape(dim // 128, 128),
            w_in_shard.T, w_out_shard,
        )

    return jax.shard_map(
        device_step,
        mesh=mesh,
        in_specs=(P("dp"), P("tp", None), P(), P(None, "tp"), P("tp", None)),
        out_specs=P(("dp", "tp"), None),
        check_vma=False,
    )
```

```python
import functools

import jax
import jax.numpy as jnp
from jax import lax
from jax.experimental import pallas as pl
from jax.experimental.pallas import tpu as pltpu
from jax.sharding import PartitionSpec as P

MESH = pl.DeviceIdType.MESH
RMS_EPS = 1e-6
CORES = 2
PIECES = 4
ROW_LAG = 1
LAG = 2
AHEAD = 3
VMEM_BYTES = 65536000


def block_kernel(
    group, ids_hbm, table_hbm, gain_hbm, w1_hbm, w2_hbm, out_ref,
    ids_ref, gain_ref, table, w1, w2, onehot, xa, xn, x_own, p1send, r1send,
    ymine, ysend, ypart, r2recv, r2send,
    load_sem, w_sem, p1_ssem, p1_rsem, r1_ssem, r1_rsem,
    ag_ssem, ag_rsem, agp_ssem, agp_rsem, yp_ssem, yp_rsem, r2_ssem, r2_rsem,
    credit_ring, credit_core, late_ring, late_core,
):
    ring = group // CORES
    me = lax.axis_index("tp")
    z, core = me // CORES, me % CORES
    step_dir = 1 - 2 * core
    nxt = lax.rem(z + step_dir + ring, ring) * CORES + core
    prv = lax.rem(z - step_dir + ring, ring) * CORES + core
    mate = z * CORES + (1 - core)

    block = out_ref.shape[0]
    piece_w = xa.shape[3]
    vocab = table_hbm.shape[0]
    vocab_pad = table.shape[0]
    tile_g = min(512, piece_w)
    tile_y = min(512, piece_w)
    tiles = piece_w * PIECES // tile_g

    def remote(src, dst, ssem, rsem, dev):
        return pltpu.make_async_remote_copy(
            src_ref=src, dst_ref=dst, send_sem=ssem, recv_sem=rsem,
            device_id={"tp": dev}, device_id_type=MESH,
        )

    def table_load(j):
        cols = pl.ds(j * tile_g, tile_g)
        return pltpu.make_async_copy(
            table_hbm.at[:, cols], table.at[pl.ds(0, vocab), cols], load_sem.at[j]
        )

    def signal(sem, dev):
        pl.semaphore_signal(sem, inc=1, device_id={"tp": dev}, device_id_type=MESH)

    barrier = pltpu.get_barrier_semaphore()
    for dev in (nxt, prv, mate):
        signal(barrier, dev)

    ids_load = pltpu.make_async_copy(ids_hbm, ids_ref, w_sem.at[2])
    gain_load = pltpu.make_async_copy(gain_hbm, gain_ref, w_sem.at[3])
    ids_load.start()
    for j in range(AHEAD):
        table_load(j).start()
    gain_load.start()

    if vocab_pad > vocab:
        table[vocab:, :] = jnp.zeros((vocab_pad - vocab, table.shape[1]), table.dtype)
    ids_load.wait()
    pl.semaphore_wait(barrier, 3)

    def w1_load():
        return pltpu.make_async_copy(w1_hbm, w1, w_sem.at[0])

    def w2_load():
        return pltpu.make_async_copy(w2_hbm, w2, w_sem.at[1])

    def p1_copy(t, h):
        return remote(
            p1send.at[h], xa.at[t, h, pl.ds(block, block)],
            p1_ssem.at[h], p1_rsem.at[t, h], mate,
        )

    def r1_copy(t, h):
        return remote(
            r1send.at[t % 2, h], xa.at[t, h, pl.ds(0, block)],
            r1_ssem.at[t % 2, h], r1_rsem.at[t, h], nxt,
        )

    def chip_back(s):
        return lax.rem(z - step_dir * s + 2 * ring, ring)

    def chip_ahead(s):
        return lax.rem(z + step_dir * s + 2 * ring, ring)

    def fill_onehot(t):
        for row, chip, c in ((0, chip_back(1 + t), core), (block, chip_ahead(1 + t), 1 - core)):
            line = ids_ref[pl.ds(chip, 1), :].astype(jnp.float32)
            lanes = lax.broadcasted_iota(jnp.int32, (block, CORES * block), 1)
            rows = lax.broadcasted_iota(jnp.int32, (block, CORES * block), 0)
            mine = jnp.where(lanes == rows + c * block, line, 0.0)
            column = jnp.sum(mine, axis=1, keepdims=True).astype(jnp.int32)
            local = column - me * vocab
            slots = lax.broadcasted_iota(jnp.int32, (block, vocab_pad), 1)
            hit = jnp.where(slots == local, 1.0, 0.0)
            onehot[pl.ds(row, block), :] = hit.astype(jnp.bfloat16)

    def gather_piece(t, h):
        for j in range(piece_w // tile_g):
            g = h * (piece_w // tile_g) + j

            @pl.when(t == 0)
            def _():
                table_load(g).wait()
                if g + AHEAD < tiles:
                    table_load(g + AHEAD).start()

            rows = jnp.dot(
                onehot[...], table[:, g * tile_g:(g + 1) * tile_g],
                preferred_element_type=jnp.float32,
            ).astype(jnp.bfloat16)
            cols = slice(j * tile_g, (j + 1) * tile_g)
            x_own[h, :, cols] = rows[:block]
            p1send[h, :, cols] = rows[block:]

    def ring1_piece(t, h):
        p1_copy(t, h).wait_recv()

        @pl.when(t >= 2)
        def _():
            r1_copy(t - 2, h).wait_send()

        @pl.when(t == 0)
        def _():
            r1send[t % 2, h] = x_own[h] + xa[t, h, block:]

        @pl.when(t >= 1)
        def _():
            r1_copy(t - 1, h).wait_recv()
            r1send[t % 2, h] = x_own[h] + xa[t, h, block:] + xa[t - 1, h, :block]

        r1_copy(t, h).start()

    def ag_copy(s, h):
        return remote(
            xa.at[s, h, pl.ds(0, block)], xa.at[s + 1, h, pl.ds(0, block)],
            ag_ssem.at[s, h], ag_rsem.at[s, h], nxt,
        )

    def agp_copy(s, h):
        return remote(
            xa.at[s, h, pl.ds(0, block)], xa.at[s, h, pl.ds(block, block)],
            agp_ssem.at[s, h], agp_rsem.at[s, h], mate,
        )

    last = ring - 1

    def row_piece(t, h):
        @pl.when(t < last)
        def _():
            ring1_piece(t, h)

        @pl.when(t == last)
        def _():
            p1_copy(last, h).wait_recv()
            r1_copy(last - 1, h).wait_recv()
            xa[0, h, :block] = x_own[h] + xa[last, h, block:] + xa[last - 1, h, :block]
            if h == 0:
                pl.semaphore_wait(credit_ring, 1)
                pl.semaphore_wait(credit_core, 1)
            ag_copy(0, h).start()
            agp_copy(0, h).start()

    def rows_step(t, carry):
        fill_onehot(t)

        @pl.when(t == last)
        def _():
            signal(credit_ring, prv)
            signal(credit_core, mate)

        @pl.when(t == 1)
        def _():
            w1_load().start()
            w2_load().start()

        for h in range(PIECES):
            @pl.when(t >= 1)
            def _():
                p1_copy(t - 1, h).wait_send()

            gather_piece(t, h)
            p1_copy(t, h).start()
            if h < ROW_LAG:
                @pl.when(t >= 1)
                def _():
                    ring1_piece(t - 1, h + PIECES - ROW_LAG)
            else:
                row_piece(t, h - ROW_LAG)
        return carry

    lax.fori_loop(0, ring, rows_step, 0)

    for h in range(PIECES - ROW_LAG, PIECES):
        row_piece(last, h)
    signal(late_ring, prv)
    signal(late_core, mate)

    def yp_copy(s, h):
        return remote(
            ysend.at[h], ypart.at[s, h],
            yp_ssem.at[h], yp_rsem.at[s, h], mate,
        )

    def r2_copy(s, h):
        return remote(
            r2send.at[s % 2, h], r2recv.at[s - 1, h],
            r2_ssem.at[s % 2, h], r2_rsem.at[s - 1, h], nxt,
        )

    gain_load.wait()
    gain = gain_ref[...].astype(jnp.float32)
    lane_w = gain.shape[1]
    tiles_n = [(h, k) for h in range(PIECES) for k in range(piece_w // lane_w)]

    def normalize(s):
        squares = jnp.zeros((2 * block, lane_w), jnp.float32)
        for h, k in tiles_n:
            xf = xa[s, h, :, k * lane_w:(k + 1) * lane_w].astype(jnp.float32)
            squares = squares + xf * xf
        mean = jnp.sum(squares, axis=-1, keepdims=True) / (piece_w * PIECES)
        inv_rms = lax.rsqrt(mean + RMS_EPS)
        for line, (h, k) in enumerate(tiles_n):
            cols = slice(k * lane_w, (k + 1) * lane_w)
            xf = xa[s, h, :, cols].astype(jnp.float32)
            xn[h, :, cols] = (xf * inv_rms * gain[line:line + 1, :]).astype(jnp.bfloat16)

    w1_load().wait()
    w2_load().wait()

    def combine(s, h):
        yp_copy(s, h).wait_recv()

        @pl.when(s >= 3)
        def _():
            r2_copy(s - 2, h).wait_send()

        @pl.when(s == 1)
        def _():
            r2send[s % 2, h] = ymine[1, h] + ypart[s, h]

        @pl.when(s >= 2)
        def _():
            r2_copy(s - 1, h).wait_recv()
            r2send[s % 2, h] = ymine[1, h] + ypart[s, h] + r2recv[s - 2, h]

        r2_copy(s, h).start()

    def pass_on(s, h):
        @pl.when(s < last)
        def _():
            ag_copy(s, h).wait_recv()
            agp_copy(s + 1, h).start()

        @pl.when(s < last - 1)
        def _():
            ag_copy(s + 1, h).start()

    def mlp_step(s, carry):
        @pl.when(s == 1)
        def _():
            pl.semaphore_wait(late_ring, 1)
            pl.semaphore_wait(late_core, 1)

        pass_on(s, 0)
        for h in range(PIECES):
            agp_copy(s, h).wait_recv()
        pass_on(s, 1)
        normalize(s)
        acc = None
        for h in range(PIECES):
            if h > 0 and h + 1 < PIECES:
                pass_on(s, h + 1)
            part = lax.dot_general(
                xn[h], w1[:, h * piece_w:(h + 1) * piece_w], (((1,), (1,)), ((), ())),
                preferred_element_type=jnp.float32,
            )
            acc = part if acc is None else acc + part
        u = acc.astype(jnp.bfloat16).astype(jnp.float32)
        act = jax.nn.gelu(u, approximate=True).astype(jnp.bfloat16)

        kept = jnp.minimum(s, 1)
        for h in range(PIECES):
            @pl.when(s >= 1)
            def _():
                yp_copy(s - 1, h).wait_send()

            for j in range(piece_w // tile_y):
                c0 = h * piece_w + j * tile_y
                y = jnp.dot(act, w2[:, c0:c0 + tile_y], preferred_element_type=jnp.float32)
                cols = slice(j * tile_y, (j + 1) * tile_y)
                ymine[kept, h, :, cols] = y[:block]
                ysend[h, :, cols] = y[block:]
            yp_copy(s, h).start()
            if h >= LAG:
                @pl.when(s >= 1)
                def _():
                    combine(s, h - LAG)

        for h in range(PIECES - LAG, PIECES):
            @pl.when(s >= 1)
            def _():
                combine(s, h)
        return carry

    lax.fori_loop(0, ring, mlp_step, 0)

    for h in range(PIECES):
        yp_copy(0, h).wait_recv()
        r2_copy(ring - 1, h).wait_recv()
        own = ymine[0, h] + ypart[0, h] + r2recv[ring - 2, h]
        out_ref[:, h * piece_w:(h + 1) * piece_w] = (
            xa[0, h, :block].astype(jnp.float32) + own
        ).astype(jnp.bfloat16)

    for h in range(PIECES):
        p1_copy(last, h).wait_send()
        yp_copy(last, h).wait_send()
        for t in (ring - 2, ring - 1):
            r1_copy(t - 1, h).wait_send()
            r2_copy(t, h).wait_send()
        for s in range(ring):
            agp_copy(s, h).wait_send()
            if s < ring - 1:
                ag_copy(s, h).wait_send()


def solution(mesh):
    group = mesh.shape["tp"]
    ring = group // CORES

    def device_step(token_ids, table_shard, norm_gain, w_in_shard, w_out_shard):
        tokens = token_ids.shape[0]
        vocab, dim = table_shard.shape
        width = w_in_shard.shape[1]
        block, piece_w = tokens // group, dim // PIECES
        vocab_pad = -(-vocab // 256) * 256
        bf16, f32 = jnp.bfloat16, jnp.float32
        dma = pltpu.SemaphoreType.DMA
        vmem = pl.BlockSpec(memory_space=pltpu.VMEM)
        hbm = pl.BlockSpec(memory_space=pl.ANY)
        return pl.pallas_call(
            functools.partial(block_kernel, group),
            name="lookup_mlp",
            out_shape=pltpu.VMEM((block, dim), bf16),
            in_specs=[hbm] * 5,
            out_specs=vmem,
            scratch_shapes=[
                pltpu.VMEM((ring, CORES * block), jnp.int32),
                pltpu.VMEM((dim // 128, 128), bf16),
                pltpu.VMEM((vocab_pad, dim), bf16),
                pltpu.VMEM((width, dim), bf16),
                pltpu.VMEM((width, dim), bf16),
                pltpu.VMEM((2 * block, vocab_pad), bf16),
                pltpu.VMEM((ring, PIECES, 2 * block, piece_w), bf16),
                pltpu.VMEM((PIECES, 2 * block, piece_w), bf16),
                pltpu.VMEM((PIECES, block, piece_w), bf16),
                pltpu.VMEM((PIECES, block, piece_w), bf16),
                pltpu.VMEM((2, PIECES, block, piece_w), bf16),
                pltpu.VMEM((2, PIECES, block, piece_w), f32),
                pltpu.VMEM((PIECES, block, piece_w), f32),
                pltpu.VMEM((ring, PIECES, block, piece_w), f32),
                pltpu.VMEM((ring - 1, PIECES, block, piece_w), f32),
                pltpu.VMEM((2, PIECES, block, piece_w), f32),
                dma((dim // min(512, piece_w),)),
                dma((4,)),
                dma((PIECES,)), dma((ring, PIECES)),
                dma((2, PIECES)), dma((ring - 1, PIECES)),
                dma((ring, PIECES)), dma((ring, PIECES)),
                dma((ring, PIECES)), dma((ring, PIECES)),
                dma((PIECES,)), dma((ring, PIECES)),
                dma((2, PIECES)), dma((ring - 1, PIECES)),
            ] + [pltpu.SemaphoreType.REGULAR] * 4,
            compiler_params=pltpu.CompilerParams(
                collective_id=0, has_side_effects=True, vmem_limit_bytes=VMEM_BYTES
            ),
        )(
            token_ids.reshape(ring, CORES * block), table_shard, norm_gain.reshape(dim // 128, 128),
            w_in_shard.T, w_out_shard,
        )

    return jax.shard_map(
        device_step,
        mesh=mesh,
        in_specs=(P("dp"), P("tp", None), P(), P(None, "tp"), P("tp", None)),
        out_specs=P(("dp", "tp"), None),
        check_vma=False,
    )
```

```python
import functools

import jax
import jax.numpy as jnp
from jax import lax
from jax.experimental import pallas as pl
from jax.experimental.pallas import tpu as pltpu
from jax.sharding import PartitionSpec as P

MESH = pl.DeviceIdType.MESH
RMS_EPS = 1e-6
CORES = 2
PIECES = 4
ROW_LAG = 1
LAG = 2
AHEAD = 2
VMEM_BYTES = 65536000


def block_kernel(
    group, ids_hbm, table_hbm, gain_hbm, w1_hbm, w2_hbm, out_ref,
    ids_ref, gain_ref, table, w1, w2, onehot, xa, xn, x_own, p1send, r1send,
    ymine, ysend, ypart, r2recv, r2send,
    load_sem, w_sem, p1_ssem, p1_rsem, r1_ssem, r1_rsem,
    ag_ssem, ag_rsem, agp_ssem, agp_rsem, yp_ssem, yp_rsem, r2_ssem, r2_rsem,
    credit_ring, credit_core, late_ring, late_core,
):
    ring = group // CORES
    me = lax.axis_index("tp")
    z, core = me // CORES, me % CORES
    step_dir = 1 - 2 * core
    nxt = lax.rem(z + step_dir + ring, ring) * CORES + core
    prv = lax.rem(z - step_dir + ring, ring) * CORES + core
    mate = z * CORES + (1 - core)

    block = out_ref.shape[0]
    piece_w = xa.shape[3]
    vocab = table_hbm.shape[0]
    vocab_pad = table.shape[0]
    tile_g = min(512, piece_w)
    tile_y = min(512, piece_w)
    tiles = piece_w * PIECES // tile_g

    def remote(src, dst, ssem, rsem, dev):
        return pltpu.make_async_remote_copy(
            src_ref=src, dst_ref=dst, send_sem=ssem, recv_sem=rsem,
            device_id={"tp": dev}, device_id_type=MESH,
        )

    upper = vocab // 2 // 16 * 16

    def table_load(j):
        cols = pl.ds(j * tile_g, tile_g)
        return [
            pltpu.make_async_copy(
                table_hbm.at[rows, cols], table.at[rows, cols], load_sem.at[j, part]
            )
            for part, rows in enumerate((pl.ds(0, upper), pl.ds(upper, vocab - upper)))
        ]

    def signal(sem, dev):
        pl.semaphore_signal(sem, inc=1, device_id={"tp": dev}, device_id_type=MESH)

    barrier = pltpu.get_barrier_semaphore()
    for dev in (nxt, prv, mate):
        signal(barrier, dev)

    ids_load = pltpu.make_async_copy(ids_hbm, ids_ref, w_sem.at[2])
    gain_load = pltpu.make_async_copy(gain_hbm, gain_ref, w_sem.at[3])
    ids_load.start()
    for j in range(AHEAD):
        for copy in table_load(j):
            copy.start()
    gain_load.start()

    if vocab_pad > vocab:
        table[vocab:, :] = jnp.zeros((vocab_pad - vocab, table.shape[1]), table.dtype)
    ids_load.wait()
    pl.semaphore_wait(barrier, 3)

    def w1_load():
        return pltpu.make_async_copy(w1_hbm, w1, w_sem.at[0])

    def w2_load():
        return pltpu.make_async_copy(w2_hbm, w2, w_sem.at[1])

    def p1_copy(t, h):
        return remote(
            p1send.at[h], xa.at[t, h, pl.ds(block, block)],
            p1_ssem.at[h], p1_rsem.at[t, h], mate,
        )

    def r1_copy(t, h):
        return remote(
            r1send.at[t % 2, h], xa.at[t, h, pl.ds(0, block)],
            r1_ssem.at[t % 2, h], r1_rsem.at[t, h], nxt,
        )

    def chip_back(s):
        return lax.rem(z - step_dir * s + 2 * ring, ring)

    def chip_ahead(s):
        return lax.rem(z + step_dir * s + 2 * ring, ring)

    def fill_onehot(t):
        for row, chip, c in ((0, chip_back(1 + t), core), (block, chip_ahead(1 + t), 1 - core)):
            line = ids_ref[pl.ds(chip, 1), :].astype(jnp.float32)
            lanes = lax.broadcasted_iota(jnp.int32, (block, CORES * block), 1)
            rows = lax.broadcasted_iota(jnp.int32, (block, CORES * block), 0)
            mine = jnp.where(lanes == rows + c * block, line, 0.0)
            column = jnp.sum(mine, axis=1, keepdims=True).astype(jnp.int32)
            local = column - me * vocab
            slots = lax.broadcasted_iota(jnp.int32, (block, vocab_pad), 1)
            hit = jnp.where(slots == local, 1.0, 0.0)
            onehot[pl.ds(row, block), :] = hit.astype(jnp.bfloat16)

    def gather_piece(t, h):
        for j in range(piece_w // tile_g):
            g = h * (piece_w // tile_g) + j

            @pl.when(t == 0)
            def _():
                if g + AHEAD < tiles:
                    for copy in table_load(g + AHEAD):
                        copy.start()
                for copy in table_load(g):
                    copy.wait()

            rows = jnp.dot(
                onehot[...], table[:, g * tile_g:(g + 1) * tile_g],
                preferred_element_type=jnp.float32,
            ).astype(jnp.bfloat16)
            cols = slice(j * tile_g, (j + 1) * tile_g)
            x_own[h, :, cols] = rows[:block]
            p1send[h, :, cols] = rows[block:]

    def ring1_piece(t, h):
        p1_copy(t, h).wait_recv()

        @pl.when(t >= 2)
        def _():
            r1_copy(t - 2, h).wait_send()

        @pl.when(t == 0)
        def _():
            r1send[t % 2, h] = x_own[h] + xa[t, h, block:]

        @pl.when(t >= 1)
        def _():
            r1_copy(t - 1, h).wait_recv()
            r1send[t % 2, h] = x_own[h] + xa[t, h, block:] + xa[t - 1, h, :block]

        r1_copy(t, h).start()

    def ag_copy(s, h):
        return remote(
            xa.at[s, h, pl.ds(0, block)], xa.at[s + 1, h, pl.ds(0, block)],
            ag_ssem.at[s, h], ag_rsem.at[s, h], nxt,
        )

    def agp_copy(s, h):
        return remote(
            xa.at[s, h, pl.ds(0, block)], xa.at[s, h, pl.ds(block, block)],
            agp_ssem.at[s, h], agp_rsem.at[s, h], mate,
        )

    last = ring - 1

    def row_piece(t, h):
        @pl.when(t < last)
        def _():
            ring1_piece(t, h)

        @pl.when(t == last)
        def _():
            p1_copy(last, h).wait_recv()
            r1_copy(last - 1, h).wait_recv()
            xa[0, h, :block] = x_own[h] + xa[last, h, block:] + xa[last - 1, h, :block]
            if h == 0:
                pl.semaphore_wait(credit_ring, 1)
                pl.semaphore_wait(credit_core, 1)
            ag_copy(0, h).start()
            agp_copy(0, h).start()

    def rows_step(t, carry):
        fill_onehot(t)

        @pl.when(t == last)
        def _():
            signal(credit_ring, prv)
            signal(credit_core, mate)

        @pl.when(t == 1)
        def _():
            w1_load().start()
            w2_load().start()

        for h in range(PIECES):
            @pl.when(t >= 1)
            def _():
                p1_copy(t - 1, h).wait_send()

            gather_piece(t, h)
            p1_copy(t, h).start()
            if h < ROW_LAG:
                @pl.when(t >= 1)
                def _():
                    ring1_piece(t - 1, h + PIECES - ROW_LAG)
            else:
                row_piece(t, h - ROW_LAG)
        return carry

    lax.fori_loop(0, ring, rows_step, 0)

    for h in range(PIECES - ROW_LAG, PIECES):
        row_piece(last, h)
    signal(late_ring, prv)
    signal(late_core, mate)

    def yp_copy(s, h):
        return remote(
            ysend.at[h], ypart.at[s, h],
            yp_ssem.at[h], yp_rsem.at[s, h], mate,
        )

    def r2_copy(s, h):
        return remote(
            r2send.at[s % 2, h], r2recv.at[s - 1, h],
            r2_ssem.at[s % 2, h], r2_rsem.at[s - 1, h], nxt,
        )

    gain_load.wait()
    gain = gain_ref[...].astype(jnp.float32)
    lane_w = gain.shape[1]
    tiles_n = [(h, k) for h in range(PIECES) for k in range(piece_w // lane_w)]

    def normalize(s):
        squares = jnp.zeros((2 * block, lane_w), jnp.float32)
        for h, k in tiles_n:
            xf = xa[s, h, :, k * lane_w:(k + 1) * lane_w].astype(jnp.float32)
            squares = squares + xf * xf
        mean = jnp.sum(squares, axis=-1, keepdims=True) / (piece_w * PIECES)
        inv_rms = lax.rsqrt(mean + RMS_EPS)
        for line, (h, k) in enumerate(tiles_n):
            cols = slice(k * lane_w, (k + 1) * lane_w)
            xf = xa[s, h, :, cols].astype(jnp.float32)
            xn[h, :, cols] = (xf * inv_rms * gain[line:line + 1, :]).astype(jnp.bfloat16)

    w1_load().wait()
    w2_load().wait()

    def combine(s, h):
        yp_copy(s, h).wait_recv()

        @pl.when(s >= 3)
        def _():
            r2_copy(s - 2, h).wait_send()

        @pl.when(s == 1)
        def _():
            r2send[s % 2, h] = ymine[1, h] + ypart[s, h]

        @pl.when(s >= 2)
        def _():
            r2_copy(s - 1, h).wait_recv()
            r2send[s % 2, h] = ymine[1, h] + ypart[s, h] + r2recv[s - 2, h]

        r2_copy(s, h).start()

    def pass_on(s, h):
        @pl.when(s < last)
        def _():
            ag_copy(s, h).wait_recv()
            agp_copy(s + 1, h).start()

        @pl.when(s < last - 1)
        def _():
            ag_copy(s + 1, h).start()

    def mlp_step(s, carry):
        @pl.when(s == 1)
        def _():
            pl.semaphore_wait(late_ring, 1)
            pl.semaphore_wait(late_core, 1)

        pass_on(s, 0)
        for h in range(PIECES):
            agp_copy(s, h).wait_recv()
        pass_on(s, 1)
        normalize(s)
        acc = None
        for h in range(PIECES):
            if h > 0 and h + 1 < PIECES:
                pass_on(s, h + 1)
            part = lax.dot_general(
                xn[h], w1[:, h * piece_w:(h + 1) * piece_w], (((1,), (1,)), ((), ())),
                preferred_element_type=jnp.float32,
            )
            acc = part if acc is None else acc + part
        u = acc.astype(jnp.bfloat16).astype(jnp.float32)
        act = jax.nn.gelu(u, approximate=True).astype(jnp.bfloat16)

        kept = jnp.minimum(s, 1)
        for h in range(PIECES):
            @pl.when(s >= 1)
            def _():
                yp_copy(s - 1, h).wait_send()

            for j in range(piece_w // tile_y):
                c0 = h * piece_w + j * tile_y
                y = jnp.dot(act, w2[:, c0:c0 + tile_y], preferred_element_type=jnp.float32)
                cols = slice(j * tile_y, (j + 1) * tile_y)
                ymine[kept, h, :, cols] = y[:block]
                ysend[h, :, cols] = y[block:]
            yp_copy(s, h).start()
            if h >= LAG:
                @pl.when(s >= 1)
                def _():
                    combine(s, h - LAG)

        for h in range(PIECES - LAG, PIECES):
            @pl.when(s >= 1)
            def _():
                combine(s, h)
        return carry

    lax.fori_loop(0, ring, mlp_step, 0)

    for h in range(PIECES):
        yp_copy(0, h).wait_recv()
        r2_copy(ring - 1, h).wait_recv()
        own = ymine[0, h] + ypart[0, h] + r2recv[ring - 2, h]
        out_ref[:, h * piece_w:(h + 1) * piece_w] = (
            xa[0, h, :block].astype(jnp.float32) + own
        ).astype(jnp.bfloat16)

    for h in range(PIECES):
        p1_copy(last, h).wait_send()
        yp_copy(last, h).wait_send()
        for t in (ring - 2, ring - 1):
            r1_copy(t - 1, h).wait_send()
            r2_copy(t, h).wait_send()
        for s in range(ring):
            agp_copy(s, h).wait_send()
            if s < ring - 1:
                ag_copy(s, h).wait_send()


def solution(mesh):
    group = mesh.shape["tp"]
    ring = group // CORES

    def device_step(token_ids, table_shard, norm_gain, w_in_shard, w_out_shard):
        tokens = token_ids.shape[0]
        vocab, dim = table_shard.shape
        width = w_in_shard.shape[1]
        block, piece_w = tokens // group, dim // PIECES
        vocab_pad = -(-vocab // 256) * 256
        bf16, f32 = jnp.bfloat16, jnp.float32
        dma = pltpu.SemaphoreType.DMA
        vmem = pl.BlockSpec(memory_space=pltpu.VMEM)
        hbm = pl.BlockSpec(memory_space=pl.ANY)
        return pl.pallas_call(
            functools.partial(block_kernel, group),
            name="lookup_mlp",
            out_shape=pltpu.VMEM((block, dim), bf16),
            in_specs=[hbm] * 5,
            out_specs=vmem,
            scratch_shapes=[
                pltpu.VMEM((ring, CORES * block), jnp.int32),
                pltpu.VMEM((dim // 128, 128), bf16),
                pltpu.VMEM((vocab_pad, dim), bf16),
                pltpu.VMEM((width, dim), bf16),
                pltpu.VMEM((width, dim), bf16),
                pltpu.VMEM((2 * block, vocab_pad), bf16),
                pltpu.VMEM((ring, PIECES, 2 * block, piece_w), bf16),
                pltpu.VMEM((PIECES, 2 * block, piece_w), bf16),
                pltpu.VMEM((PIECES, block, piece_w), bf16),
                pltpu.VMEM((PIECES, block, piece_w), bf16),
                pltpu.VMEM((2, PIECES, block, piece_w), bf16),
                pltpu.VMEM((2, PIECES, block, piece_w), f32),
                pltpu.VMEM((PIECES, block, piece_w), f32),
                pltpu.VMEM((ring, PIECES, block, piece_w), f32),
                pltpu.VMEM((ring - 1, PIECES, block, piece_w), f32),
                pltpu.VMEM((2, PIECES, block, piece_w), f32),
                dma((dim // min(512, piece_w), 2)),
                dma((4,)),
                dma((PIECES,)), dma((ring, PIECES)),
                dma((2, PIECES)), dma((ring - 1, PIECES)),
                dma((ring, PIECES)), dma((ring, PIECES)),
                dma((ring, PIECES)), dma((ring, PIECES)),
                dma((PIECES,)), dma((ring, PIECES)),
                dma((2, PIECES)), dma((ring - 1, PIECES)),
            ] + [pltpu.SemaphoreType.REGULAR] * 4,
            compiler_params=pltpu.CompilerParams(
                collective_id=0, has_side_effects=True, vmem_limit_bytes=VMEM_BYTES
            ),
        )(
            token_ids.reshape(ring, CORES * block), table_shard, norm_gain.reshape(dim // 128, 128),
            w_in_shard.T, w_out_shard,
        )

    return jax.shard_map(
        device_step,
        mesh=mesh,
        in_specs=(P("dp"), P("tp", None), P(), P(None, "tp"), P("tp", None)),
        out_specs=P(("dp", "tp"), None),
        check_vma=False,
    )
```
